32 devices in a mesh: grid: 8 (over y, x, core), band: 4 (over z).
Axes of the slice: x: 2, y: 2, z: 4, core: 2. Of those that a mesh axis runs over, the one named last changes fastest.
Arguments:
- start: float32 [1, 4, 1, 64, 32768], P(None, None, None, 'band', 'grid'), may hold values from -6 to 6
- energies: float32 [4, 64, 32768], P(None, 'band', 'grid'), may hold values from -4 to 4
- sites: int32 [3, 1], replicated, may hold values from 0 to 31
- potential: float32 [32, 32, 32], replicated, may hold values from -4 to 400
Outputs:
- alphas: float32 [1, 1, 4], replicated
- betas: float32 [1, 1, 4], replicated
- lanczos: float32 [1, 4, 1, 64, 32768], P(None, None, None, 'band', 'grid')
The draws below stay inside these ranges and needn't reach their ends.
All inputs are finite; a program needn't handle non-finite values.
Results may differ from the reference program's by a relative error of at most 0.0003.
Values sent between devices are 32-bit elements; how exact they have to be, the bound alone decides.
A program may use at most 64 MiB of HBM per device.

```python
import jax
import jax.numpy as jnp
from jax import lax

GRIDN = 32
CBANDS = 64
CORES = 4
POLS = 1
ITERS = 4
ATOMS = 1
KPOINTS = 32768


def draw_potential(key, part):
    first, second = jax.random.split(key)
    coords = jnp.arange(GRIDN, dtype=jnp.int32)
    distance = jnp.minimum(coords, GRIDN - coords).astype(jnp.float32)
    square = distance[:, None, None] ** 2 + distance[None, :, None] ** 2 + distance[None, None, :] ** 2
    radius = jnp.sqrt(square)
    spread_cells, height, tail_charge, background = (1.5, 250.0, 6.0, 3.0)
    roughness = jax.random.uniform(first, (GRIDN, GRIDN, GRIDN), jnp.float32, 0.5, 1.5)
    jitter = jax.random.uniform(second, (GRIDN, GRIDN, GRIDN), jnp.float32, -1.0, 1.0)
    peaked = height * jnp.exp(-square / (2.0 * spread_cells * spread_cells)) * roughness
    screened_tail = tail_charge / jnp.maximum(radius, 0.5)
    return peaked + screened_tail + background * jitter


def block_scale(rng, extent, shards, least, top_value):
    def one(position, parts):
        steps = jax.random.uniform(jax.random.fold_in(jax.random.fold_in(rng, 6), position), (parts,), jnp.float32, least / len(shards), top_value / len(shards))
        return jnp.repeat(jnp.exp(steps), extent[position] // parts).reshape((-1,) + (1,) * (len(extent) - position - 1))

    gain = one(*shards[0])
    for cut in shards[1:]:
        gain = gain * one(*cut)
    return gain


def scatter_about(key, extent, spread, reach, pieces=(), kind=jnp.bfloat16):
    array = spread * jax.random.normal(key, extent, jnp.float32)
    if pieces:
        array = array * block_scale(key, extent, pieces, -0.22, 0.18)
    return jnp.clip(array, -reach, reach).astype(kind)


def setup_inputs(seed: int = 0) -> dict:
    splits = jax.random.split(jax.random.key(seed), 5)
    start = scatter_about(splits[0], (ATOMS, CORES, POLS, CBANDS, KPOINTS), 1.0, 6.0, ((3, 4), (4, 8)), jnp.float32)
    energies = jnp.clip(jax.random.uniform(splits[1], (CORES, CBANDS, KPOINTS), jnp.float32, -4.0, 4.0) * block_scale(splits[1], (CORES, CBANDS, KPOINTS), ((1, 4), (2, 8)), -0.4, 0.0), -4.0, 4.0)
    sites = jax.random.randint(splits[2], (3, ATOMS), 0, GRIDN).astype(jnp.int32)
    potential = draw_potential(jax.random.fold_in(splits[4], 71), 0)
    return dict(start=start, energies=energies, sites=sites, potential=potential)


def cas_along(field_part, axis_number):
    spectrum = jnp.fft.fft(field_part, axis=axis_number)
    return (spectrum.real - spectrum.imag).astype(field_part.dtype)

def cas_three(field_part):
    return cas_along(cas_along(cas_along(field_part, 1), 2), 3)

def shift_axis(field_part, offset, axis_number):
    length = field_part.shape[axis_number]
    doubled = jnp.concatenate([field_part, field_part], axis=axis_number)
    first_index = ((length - offset) % length).astype(jnp.int32)
    return lax.dynamic_slice_in_dim(doubled, first_index, length, axis_number)

def reference(start, energies, sites, potential):
    grid_size = potential.shape[0]
    volume = grid_size * grid_size * grid_size
    shifted_list = []
    for atom_index in range(ATOMS):
        shifted = shift_axis(potential, sites[0, atom_index], 0)
        shifted = shift_axis(shifted, sites[1, atom_index], 1)
        shifted = shift_axis(shifted, sites[2, atom_index], 2)
        shifted_list.append(shifted)
    weights_all = jnp.repeat(jnp.stack(shifted_list), CORES, axis=0)

    def per_block(pair_items):
        field_block, weights = pair_items
        return cas_three(weights[None] * cas_three(field_block)) / volume

    def direct(vector):
        flat_vec = vector.reshape(ATOMS * CORES, POLS * CBANDS, grid_size, grid_size, grid_size)
        result = lax.map(per_block, (flat_vec, weights_all))
        return result.reshape(vector.shape)
    total_count = CORES * CBANDS * KPOINTS

    def inner(left, right):
        return lax.optimization_barrier(jnp.sum(left * right, axis=(1, 3, 4))) / total_count

    def expand_coef(values):
        return values[:, None, :, None, None]
    lanczos = start / expand_coef(jnp.sqrt(inner(start, start)))
    previous = jnp.zeros_like(start)
    beta_prev = jnp.zeros((ATOMS, POLS), jnp.float32)
    alpha_list = []
    beta_list = []
    for iteration in range(ITERS):
        applied = energies[None, :, None] * lanczos - direct(lanczos)
        alpha_now = inner(lanczos, applied)
        remainder = applied - expand_coef(alpha_now) * lanczos - expand_coef(beta_prev) * previous
        beta_now = jnp.sqrt(inner(remainder, remainder))
        previous = lanczos
        lanczos = remainder / expand_coef(beta_now)
        beta_prev = beta_now
        alpha_list.append(alpha_now)
        beta_list.append(beta_now)
    return (jnp.stack(alpha_list, axis=2), jnp.stack(beta_list, axis=2), lanczos)
```

```python
import functools
import math

import jax
import jax.numpy as jnp
import numpy as np
from jax import lax
from jax.experimental import pallas as pl
from jax.experimental.pallas import tpu as pltpu
from jax.sharding import PartitionSpec as P

ITERS = 4


precise_mode = lax.Precision.HIGHEST


def cas_table(grid_size):
    cells = jnp.arange(grid_size, dtype=jnp.int32)
    phase = cells[:, None] * cells[None, :] % grid_size
    angle = phase.astype(jnp.float32) * (2.0 * math.pi / grid_size)
    return jnp.cos(angle) + jnp.sin(angle)


def shift_axis(field_part, offset, axis_number):
    length = field_part.shape[axis_number]
    doubled = jnp.concatenate([field_part, field_part], axis=axis_number)
    first_index = (length - offset) % length
    return lax.dynamic_slice_in_dim(doubled, first_index, length, axis_number)


def expand_coef(values):
    return values[:, None, :, None, None]


def plane_body(start, energies, sites, potential):
    grid_size = potential.shape[0]
    volume = grid_size * grid_size * grid_size
    atom_count, core_count, pol_count, band_local, kpoint_local = start.shape
    plane_count = grid_size // lax.axis_size("grid")
    position = lax.axis_index("grid")
    chain_count = core_count * pol_count * band_local
    field_count = atom_count * chain_count
    total_count = (
        core_count * band_local * lax.axis_size("band") * kpoint_local * lax.axis_size("grid")
    )
    cas_grid = cas_table(grid_size)
    shifted = shift_axis(potential, sites[0, 0], 0)
    shifted = shift_axis(shifted, sites[1, 0], 1)
    shifted = shift_axis(shifted, sites[2, 0], 2)
    tables = [shifted]
    shifted_all = jnp.stack(tables, axis=-1)
    slab_table = lax.dynamic_slice_in_dim(shifted_all, position * plane_count, plane_count, 1)

    def moment(left, right):
        return jnp.sum(left * right, axis=(1, 3, 4)) / total_count

    start_sum = lax.psum(moment(start, start), ("grid", "band"))
    lanczos = start / expand_coef(jnp.sqrt(start_sum))
    previous = jnp.zeros_like(start)
    beta_prev = jnp.zeros((atom_count, pol_count), jnp.float32)
    alpha_list = []
    beta_list = []
    for iteration in range(ITERS):
        spread_fields = lanczos.reshape(atom_count, chain_count, plane_count, grid_size, grid_size)
        spread_over_z = jnp.einsum(
            "arpyz,wz->pywar", spread_fields, cas_grid, precision=precise_mode
        )
        spread_over_y = jnp.einsum(
            "pywar,uy->puwar", spread_over_z, cas_grid, precision=precise_mode
        )
        direct_spectrum = lax.all_to_all(
            spread_over_y.reshape(plane_count, grid_size, grid_size, field_count),
            "grid",
            split_axis=1,
            concat_axis=0,
            tiled=True,
        )
        field_shape = direct_spectrum.shape
        over_x = jnp.einsum("xvwf,tx->tvwf", direct_spectrum, cas_grid, precision=precise_mode)
        split_view = over_x.reshape(
            field_shape[0], field_shape[1], field_shape[2], atom_count, chain_count
        )
        scaled = split_view * slab_table[..., None]
        back_x = jnp.einsum("tvwar,xt->xvwar", scaled, cas_grid, precision=precise_mode)
        weighted = back_x.reshape(field_shape)
        direct_returned = lax.all_to_all(weighted, "grid", split_axis=0, concat_axis=1, tiled=True)
        fields = direct_returned.reshape(plane_count, grid_size, grid_size, atom_count, chain_count)
        over_z = jnp.einsum("pvwar,zw->pvzar", fields, cas_grid, precision=precise_mode)
        over_y = jnp.einsum("pvzar,yv->arpyz", over_z, cas_grid, precision=precise_mode)
        applied = energies[None, :, None] * lanczos - over_y.reshape(start.shape) / volume
        moments_all = lax.psum(
            (
                moment(lanczos, applied),
                moment(applied, applied),
                moment(lanczos, lanczos),
                moment(previous, previous),
                moment(previous, applied),
                moment(lanczos, previous),
            ),
            ("grid", "band"),
        )
        alpha_now = moments_all[0]
        square = (
            moments_all[1]
            + alpha_now * alpha_now * moments_all[2]
            + beta_prev * beta_prev * moments_all[3]
        )
        square = square - 2.0 * alpha_now * moments_all[0] - 2.0 * beta_prev * moments_all[4]
        square = square + 2.0 * alpha_now * beta_prev * moments_all[5]
        beta_now = jnp.sqrt(square)
        remainder = applied - expand_coef(alpha_now) * lanczos - expand_coef(beta_prev) * previous
        previous = lanczos
        lanczos = remainder / expand_coef(beta_now)
        beta_prev = beta_now
        alpha_list.append(alpha_now)
        beta_list.append(beta_now)
    return (jnp.stack(alpha_list, axis=2), jnp.stack(beta_list, axis=2), lanczos)


MESH = pl.DeviceIdType.MESH
LANES = 128
SUBLANES = 8
GROUPS = 2
PART = SUBLANES // GROUPS


def split(value):
    high = value.astype(jnp.bfloat16)
    return high, (value - high.astype(jnp.float32)).astype(jnp.bfloat16)


def dot3(left, right):
    left_high, left_low = left
    right_high, right_low = right
    left = jnp.concatenate([left_high, left_low, left_high], axis=1)
    right = jnp.concatenate([right_high, right_high, right_low], axis=0)
    return jnp.dot(left, right, preferred_element_type=jnp.float32)


def shifted_potential(table, sites, grid_size):
    cells = grid_size * grid_size
    lane = lax.broadcasted_iota(jnp.int32, table.shape, 1) % grid_size
    for axis in range(3):
        step = 1
        while step < grid_size:
            if axis == 0:
                moved = pltpu.roll(table, step, 0)
            elif axis == 1:
                moved = pltpu.roll(table, step * grid_size, 1)
            else:
                moved = jnp.where(
                    lane >= step,
                    pltpu.roll(table, step, 1),
                    pltpu.roll(table, cells - grid_size + step, 1),
                )
            flag = jnp.full(table.shape, sites[axis] // step % 2, jnp.int32)
            table = jnp.where(flag == 1, moved, table)
            step *= 2
    return table


def total_of(parts):
    total = parts[0]
    for part in parts[1:]:
        total = total + part
    return jnp.sum(jnp.sum(total, axis=0, keepdims=True), axis=1, keepdims=True)


def inverse_of(value):
    return jnp.where(value > 0.0, 1.0 / jnp.where(value > 0.0, value, 1.0), 0.0)


def frequency_order(grid_size):
    cells = np.arange(grid_size)
    return np.concatenate([cells[0::4], cells[2::4], cells[1::2]])


def recursion_kernel(
    sizes, start, energies, sites, pot, forward_y, back_y, all_z, x_far,
    land, coef,
    forward_y_here, back_y_here, all_z_here, x_wide, pot_here, pot_flat, pot_order,
    start_here, energy_here, packed, basis, energy, site_table,
    to_high, to_low, from_high, from_low, vec_high, vec_low, mid_high, mid_low,
    outgoing, sums, gathered,
    table_sem, load_sem, send_sem, recv_sem, out_send, out_recv, sum_send, sum_recv,
):
    n, band_n, grid_size, halves = sizes
    me = lax.axis_index("grid")
    rank = lax.axis_index("band") * n + me
    members = n * band_n
    cells = grid_size * grid_size
    planes = grid_size // n
    rows = grid_size * PART
    piece = planes * PART
    quarter = cells // 4
    total_count = float(grid_size * SUBLANES * cells * members)

    load_copies = [
        pltpu.make_async_copy(source, target, load_sem.at[i])
        for i, (source, target) in enumerate(((start, start_here), (energies, energy_here)))
    ]
    table_copies = [
        pltpu.make_async_copy(source, target, table_sem.at[i])
        for i, (source, target) in enumerate((
            (forward_y, forward_y_here), (back_y, back_y_here), (all_z, all_z_here), (x_far, x_wide), (pot, pot_here)))
    ]
    for copy in load_copies + table_copies:
        copy.start()
    barrier = pltpu.get_barrier_semaphore()
    for k in range(1, members):
        peer = (rank + k) % members
        pl.semaphore_signal(barrier, inc=1, device_id={"grid": peer % n, "band": peer // n}, device_id_type=MESH)

    upper = lax.broadcasted_iota(jnp.int32, (SUBLANES, cells), 0) < PART

    def pack(kind):
        def pack_owner(owner, carry):
            at = pl.ds(pl.multiple_of(owner % halves * SUBLANES, SUBLANES), SUBLANES)
            for pair in range(planes // 2):
                first, second = slice(2 * pair * cells, (2 * pair + 1) * cells), slice((2 * pair + 1) * cells, (2 * pair + 2) * cells)
                if kind == 0:
                    one, two = start_here[0, owner // halves, 0, at, first], start_here[0, owner // halves, 0, at, second]
                else:
                    one, two = energy_here[owner // halves, at, first], energy_here[owner // halves, at, second]
                here = slice(pair * SUBLANES, (pair + 1) * SUBLANES)
                packed[kind, 0, owner, here, :] = jnp.where(upper, one, pltpu.roll(two, PART, 0))
                packed[kind, 1, owner, here, :] = jnp.where(upper, pltpu.roll(one, PART, 0), two)
            return carry

        lax.fori_loop(0, n, pack_owner, 0)

    my_rows = pl.ds(pl.multiple_of(me * piece, piece), piece)

    def piece_copy(kind, group, k):
        peer = (me + k) % n
        target = basis.at[group, 0, my_rows, :] if kind == 0 else energy.at[group, my_rows, :]
        return pltpu.make_async_remote_copy(
            src_ref=packed.at[kind, group, peer], dst_ref=target, send_sem=send_sem.at[kind, group, k],
            recv_sem=recv_sem.at[kind, group, k], device_id={"grid": peer}, device_id_type=MESH)

    load_copies[0].wait()
    pack(0)
    load_copies[1].wait()
    pack(1)
    pl.semaphore_wait(barrier, members - 1)
    for group in range(GROUPS):
        for kind in range(2):
            for k in range(1, n):
                piece_copy(kind, group, k).start()
    for group in range(GROUPS):
        basis[group, 0, my_rows, :] = packed[0, group, me]
        energy[group, my_rows, :] = packed[1, group, me]

    for copy in table_copies:
        copy.wait()

    def forward_rows(y, carry):
        high, low = split(forward_y_here[pl.ds(y, 1), :] * all_z_here[...])
        at = pl.ds(pl.multiple_of(y * grid_size, grid_size), grid_size)
        to_high[at, :] = high
        to_low[at, :] = low
        return carry

    def back_rows(v, carry):
        high, low = split(back_y_here[pl.ds(v, 1), :] * all_z_here[:, : 2 * quarter])
        at = pl.ds(pl.multiple_of(v * grid_size, grid_size), grid_size)
        from_high[at, :] = high
        from_low[at, :] = low
        return carry

    lax.fori_loop(0, grid_size // 2, forward_rows, 0)
    lax.fori_loop(0, grid_size, back_rows, 0)
    for y in range(grid_size):
        pot_flat[:, y * grid_size:(y + 1) * grid_size] = pot_here[:, y, :]
    pot_flat[...] = shifted_potential(pot_flat[...], sites, grid_size) * (1.0 / (grid_size * cells))
    for place, v in enumerate(frequency_order(grid_size)):
        pot_order[:, place * grid_size:(place + 1) * grid_size] = pot_flat[:, int(v) * grid_size:(int(v) + 1) * grid_size]
    for x in range(grid_size):
        site_table[PART * x:PART * (x + 1), :] = jnp.broadcast_to(pot_order[x:x + 1, :], (PART, cells))

    quarters = [slice(i * quarter, (i + 1) * quarter) for i in range(4)]
    odd = slice(2 * quarter, 4 * quarter)
    lane = lax.broadcasted_iota(jnp.int32, (1, LANES), 1)
    tall = 2 * SUBLANES

    def lane_is(place):
        return lane == jnp.full((1, LANES), place, jnp.int32)

    def folded(product):
        return sum((product[i:i + SUBLANES] for i in range(SUBLANES, product.shape[0], SUBLANES)), product[:SUBLANES])

    def times_x(value):
        high, low = split(value)
        return jnp.dot(x_wide[...], jnp.concatenate([high, high, low], axis=0), preferred_element_type=jnp.float32)

    def message_copy(stage, k):
        peer = (rank + k) % members
        return pltpu.make_async_remote_copy(
            src_ref=sums.at[stage, rank], dst_ref=sums.at[stage, rank], send_sem=sum_send.at[stage, k],
            recv_sem=sum_recv.at[stage, k], device_id={"grid": peer % n, "band": peer // n}, device_id_type=MESH)

    def send_message(stage, message):
        sums[stage, rank] = message
        for k in range(1, members):
            message_copy(stage, k).start()

    def step(t, carry):
        alpha, gamma, norm_before, message = carry
        group, j = t // ITERS, t % ITERS
        before, earlier = jnp.maximum(j - 1, 0), jnp.maximum(j - 2, 0)

        @pl.when(j == 0)
        def _():
            for k in range(1, n):
                piece_copy(0, group, k).wait_recv()

        norm_parts = []
        for r in range(0, rows, tall):
            at = slice(r, r + tall)
            q = []
            for cols in quarters:
                value = basis[group, j, at, cols] - alpha * basis[group, before, at, cols] - gamma * basis[group, earlier, at, cols]
                basis[group, j, at, cols] = value
                q.append(value)
            norm_parts.append(folded(q[0] * q[0] + q[1] * q[1] + q[2] * q[2] + q[3] * q[3]))
            even, other = q[0] + q[2], q[1] + q[3]
            for cols, value in zip(quarters, (even + other, even - other, q[0] - q[2], q[1] - q[3])):
                vec_high[at, cols], vec_low[at, cols] = split(value)
        for cols, depth in ((quarters[0], quarter), (quarters[1], quarter), (odd, 2 * quarter)):
            spectrum = dot3((vec_high[:, cols], vec_low[:, cols]), (to_high[:depth, cols], to_low[:depth, cols]))
            spectrum = times_x(spectrum) * site_table[:, cols]
            mid_high[:, cols], mid_low[:, cols] = split(times_x(spectrum))
        norm = total_of(norm_parts)

        @pl.when(j == 0)
        def _():
            for k in range(1, n):
                piece_copy(1, group, k).wait_recv()

        def back(at, cols):
            return dot3((mid_high[:, at], mid_low[:, at]), (from_high[at, cols], from_low[at, cols]))

        zero, two = back(quarters[0], slice(0, quarter)), back(quarters[1], slice(0, quarter))
        odds = back(odd, slice(0, 2 * quarter))
        plus, minus = zero + two, zero - two
        one, three = odds[:, :quarter], odds[:, quarter:]
        alpha_parts, square_parts = [], []
        for cols, value in zip(quarters, (plus + one, minus + three, plus - one, minus - three)):
            here = basis[group, j, :, cols]
            new = energy[group, :, cols] * here - value
            basis[group, j + 1, :, cols] = new
            alpha_parts.append(folded(here * new))
            square_parts.append(folded(new * new))
        alpha = total_of(alpha_parts) * inverse_of(norm)
        gamma = jnp.where(jnp.full((1, 1), j, jnp.int32) == 0, 0.0, norm * inverse_of(norm_before))
        norm_after = jnp.maximum(total_of(square_parts) - alpha * alpha * norm - gamma * norm, 0.0)
        place = SUBLANES * group + j
        message = jnp.where(lane_is(place), norm, message)
        message = jnp.where(lane_is(place + 1), norm_after, message)
        message = jnp.where(lane_is(place + LANES // 2), alpha, message)

        @pl.when(t == GROUPS * ITERS - 2)
        def _():
            send_message(0, message)

        keep = jnp.where(jnp.full((1, 1), j, jnp.int32) == ITERS - 1, 0.0, 1.0)
        return alpha * keep, gamma * keep, norm, message

    nothing = jnp.zeros((1, 1), jnp.float32)
    message = lax.fori_loop(0, GROUPS * ITERS, step, (nothing, nothing, nothing, jnp.zeros((1, LANES), jnp.float32)))[3]
    send_message(1, message)

    def tables_of(stage):
        for k in range(1, members):
            message_copy(stage, k).wait_recv()
        for r in range(members):
            gathered[stage, r:r + 1, :] = sums[stage, r]
        table = gathered[stage]
        norms = jnp.where(wide_lane < LANES // 2, table, 0.0)
        return norms, pltpu.roll(table, LANES // 2, 1), jnp.where(order > 0, norms * inverse_of(pltpu.roll(norms, 1, 1)), 0.0)

    wide_lane = lax.broadcasted_iota(jnp.int32, (members, LANES), 1)
    order = wide_lane % SUBLANES
    used = jnp.logical_and(order <= ITERS, wide_lane < SUBLANES * GROUPS)

    def inner(norms, left, right):
        return total_of([norms * left * right]) / total_count

    def global_step(tables, vector, previous, beta):
        norms, diagonal, coupling = tables
        raised = jnp.where(order > 0, pltpu.roll(vector, 1, 1), 0.0)
        lowered = jnp.where(order < ITERS, pltpu.roll(coupling * vector, LANES - 1, 1), 0.0)
        image = jnp.where(used, raised + jnp.where(order < ITERS, diagonal, 0.0) * vector + lowered, 0.0)
        alpha_now = inner(norms, vector, image)
        rest = image - alpha_now * vector - beta * previous
        beta_now = jnp.sqrt(inner(norms, rest, rest))
        return alpha_now, beta_now, rest / beta_now, vector

    alphas, betas = jnp.zeros((1, LANES), jnp.float32), jnp.zeros((1, LANES), jnp.float32)
    tables = tables_of(0)
    first = jnp.where(jnp.logical_and(used, order == 0), 1.0, 0.0)
    vector, previous, beta = first / jnp.sqrt(inner(tables[0], first, first)), jnp.zeros((members, LANES), jnp.float32), nothing
    for j in range(ITERS):
        if j == ITERS - 1:
            tables = tables_of(1)
        alpha, beta, vector, previous = global_step(tables, vector, previous, beta)
        alphas, betas = jnp.where(lane == j, alpha, alphas), jnp.where(lane == j, beta, betas)
    coef[0:1, :] = alphas
    coef[1:2, :] = betas
    norms, diagonal, coupling = tables
    top = ITERS - 1
    weights = vector - jnp.where(order == top, diagonal * pltpu.roll(vector, LANES - 1, 1), 0.0)
    weights = weights - jnp.where(order == top - 1, pltpu.roll(coupling, LANES - 1, 1) * pltpu.roll(vector, LANES - 2, 1), 0.0)
    mine = lax.broadcasted_iota(jnp.int32, (members, LANES), 0) == jnp.full((members, LANES), rank, jnp.int32)
    weights = jnp.sum(jnp.where(mine, weights, 0.0), axis=0, keepdims=True)
    scales = [
        [jnp.sum(jnp.where(lane == SUBLANES * group + i, weights, 0.0), axis=1, keepdims=True) for i in range(ITERS + 1)]
        for group in range(GROUPS)
    ]
    out_copies = []
    for k in range(1, n + 1):
        peer = (me + k) % n
        at = pl.ds(pl.multiple_of(peer * piece, piece), piece)
        for group in range(GROUPS):
            value = sum((scales[group][i] * basis[group, i, at, :] for i in range(1, ITERS + 1)), scales[group][0] * basis[group, 0, at, :])
            if k < n:
                outgoing[peer, group] = value
            else:
                land[me, group] = value
        if k < n:
            copy = pltpu.make_async_remote_copy(
                src_ref=outgoing.at[peer], dst_ref=land.at[me], send_sem=out_send.at[k], recv_sem=out_recv.at[k],
                device_id={"grid": peer}, device_id_type=MESH)
            copy.start()
            out_copies.append(copy)
    for group in range(GROUPS):
        for kind in range(2):
            for k in range(1, n):
                piece_copy(kind, group, k).wait_send()
    for stage in range(2):
        for k in range(1, members):
            message_copy(stage, k).wait_send()
    for copy in out_copies:
        copy.wait()


def unpack_kernel(halves, planes, land, coef, out, alphas, betas):
    owners, cells = land.shape[0], land.shape[3]
    upper = lax.broadcasted_iota(jnp.int32, (SUBLANES, cells), 0) < PART
    for owner in range(owners):
        at = slice(owner % halves * SUBLANES, (owner % halves + 1) * SUBLANES)
        for pair in range(planes // 2):
            here = slice(pair * SUBLANES, (pair + 1) * SUBLANES)
            one, two = land[owner, 0, here, :], land[owner, 1, here, :]
            out[0, owner // halves, 0, at, 2 * pair * cells:(2 * pair + 1) * cells] = jnp.where(upper, one, pltpu.roll(two, PART, 0))
            out[0, owner // halves, 0, at, (2 * pair + 1) * cells:(2 * pair + 2) * cells] = jnp.where(upper, pltpu.roll(one, PART, 0), two)
    alphas[0] = coef[0:1, :ITERS]
    betas[0] = coef[1:2, :ITERS]


def field_body(start, energies, sites, potential):
    grid_size = potential.shape[0]
    cells = grid_size * grid_size
    n, band_n = lax.axis_size("grid"), lax.axis_size("band")
    halves = start.shape[3] // SUBLANES
    planes = grid_size // n
    rows, piece, half_cells = grid_size * PART, planes * PART, cells // 2
    index = np.arange(grid_size)
    angle = (index[:, None] * index[None, :] % grid_size) * (2.0 * math.pi / grid_size)
    cas = np.cos(angle) + np.sin(angle)
    ordered = cas[frequency_order(grid_size)]
    half_grid = grid_size // 2
    forward_y = jnp.asarray(np.repeat(ordered.T[:half_grid], grid_size, axis=1), jnp.float32)
    back_y = jnp.asarray(np.repeat(ordered[:, :half_grid], grid_size, axis=1), jnp.float32)
    all_z = jnp.asarray(np.tile(cas, (1, grid_size)), jnp.float32)
    x_wide = np.kron(cas, np.eye(PART)).astype(np.float32)
    x_high = x_wide.astype(jnp.bfloat16)
    x_low = (x_wide - x_high.astype(np.float32)).astype(jnp.bfloat16)
    x_wide = jnp.asarray(np.concatenate([x_high, x_low, x_high], axis=1))
    vmem = pl.BlockSpec(memory_space=pltpu.VMEM)
    hbm = pl.BlockSpec(memory_space=pltpu.MemorySpace.HBM)
    f32, bf16 = jnp.float32, jnp.bfloat16
    dma = pltpu.SemaphoreType.DMA
    members = n * band_n
    land_shape = (n, GROUPS, piece, cells)
    start, energies, potential = (pltpu.with_memory_space_constraint(value, pltpu.MemorySpace.HBM) for value in (start, energies, potential))
    land, coef = pl.pallas_call(
        functools.partial(recursion_kernel, (n, band_n, grid_size, halves)),
        out_shape=(jax.ShapeDtypeStruct(land_shape, f32), jax.ShapeDtypeStruct((2, LANES), f32)),
        in_specs=[hbm, hbm, pl.BlockSpec(memory_space=pltpu.SMEM)] + [hbm] * 5,
        out_specs=(vmem, vmem),
        scratch_shapes=[
            pltpu.VMEM((half_grid, cells), f32), pltpu.VMEM((grid_size, half_cells), f32), pltpu.VMEM((grid_size, cells), f32),
            pltpu.VMEM((rows, 3 * rows), bf16), pltpu.VMEM(potential.shape, f32),
            pltpu.VMEM((grid_size, cells), f32), pltpu.VMEM((grid_size, cells), f32),
            pltpu.VMEM(start.shape, f32), pltpu.VMEM(energies.shape, f32),
            pltpu.VMEM((2, GROUPS, n, piece, cells), f32),
            pltpu.VMEM((GROUPS, ITERS + 1, rows, cells), f32), pltpu.VMEM((GROUPS, rows, cells), f32),
            pltpu.VMEM((rows, cells), f32),
            pltpu.VMEM((half_cells, cells), bf16), pltpu.VMEM((half_cells, cells), bf16),
            pltpu.VMEM((cells, half_cells), bf16), pltpu.VMEM((cells, half_cells), bf16),
            pltpu.VMEM((rows, cells), bf16), pltpu.VMEM((rows, cells), bf16),
            pltpu.VMEM((rows, cells), bf16), pltpu.VMEM((rows, cells), bf16),
            pltpu.VMEM(land_shape, f32),
            pltpu.VMEM((2, members, 1, LANES), f32), pltpu.VMEM((2, members, LANES), f32),
            dma((5,)), dma((2,)), dma((2, GROUPS, n)), dma((2, GROUPS, n)), dma((n,)), dma((n,)),
            dma((2, members)), dma((2, members)),
        ],
        compiler_params=pltpu.CompilerParams(collective_id=0, has_side_effects=True, vmem_limit_bytes=36 * 1024 * 1024),
    )(start, energies, sites[:, 0], potential, *(pltpu.with_memory_space_constraint(value, pltpu.MemorySpace.HBM) for value in (forward_y, back_y, all_z, x_wide)))
    scalar = jax.ShapeDtypeStruct((1, 1, ITERS), f32)
    out, alphas, betas = pl.pallas_call(
        functools.partial(unpack_kernel, halves, planes),
        out_shape=(jax.ShapeDtypeStruct(start.shape, f32), scalar, scalar),
        in_specs=[vmem, vmem],
        out_specs=(vmem, vmem, vmem),
        compiler_params=pltpu.CompilerParams(vmem_limit_bytes=8 * 1024 * 1024),
    )(land, coef)
    return alphas, betas, out


def body(start, energies, sites, potential):
    atoms, cores, pols, bands, _ = start.shape
    grid_size = potential.shape[0]
    n = lax.axis_size("grid")
    whole_fields = (
        atoms == 1 and pols == 1 and bands % SUBLANES == 0 and cores * bands == SUBLANES * n
        and grid_size % (2 * SUBLANES) == 0 and grid_size % (2 * n) == 0
        and grid_size * grid_size % (4 * LANES) == 0 and n * lax.axis_size("band") % SUBLANES == 0
    )
    return (field_body if whole_fields else plane_body)(start, energies, sites, potential)


def solution(mesh):
    in_specs = (P(None, None, None, "band", "grid"), P(None, "band", "grid"), P(), P())
    out_specs = (P(), P(), P(None, None, None, "band", "grid"))
    return jax.shard_map(body, mesh=mesh, in_specs=in_specs, out_specs=out_specs, check_vma=False)
```

```python
import functools
import math

import jax
import jax.numpy as jnp
import numpy as np
from jax import lax
from jax.experimental import pallas as pl
from jax.experimental.pallas import tpu as pltpu
from jax.sharding import PartitionSpec as P

ITERS = 4


precise_mode = lax.Precision.HIGHEST


def cas_table(grid_size):
    cells = jnp.arange(grid_size, dtype=jnp.int32)
    phase = cells[:, None] * cells[None, :] % grid_size
    angle = phase.astype(jnp.float32) * (2.0 * math.pi / grid_size)
    return jnp.cos(angle) + jnp.sin(angle)


def shift_axis(field_part, offset, axis_number):
    length = field_part.shape[axis_number]
    doubled = jnp.concatenate([field_part, field_part], axis=axis_number)
    first_index = (length - offset) % length
    return lax.dynamic_slice_in_dim(doubled, first_index, length, axis_number)


def expand_coef(values):
    return values[:, None, :, None, None]


def plane_body(start, energies, sites, potential):
    grid_size = potential.shape[0]
    volume = grid_size * grid_size * grid_size
    atom_count, core_count, pol_count, band_local, kpoint_local = start.shape
    plane_count = grid_size // lax.axis_size("grid")
    position = lax.axis_index("grid")
    chain_count = core_count * pol_count * band_local
    field_count = atom_count * chain_count
    total_count = (
        core_count * band_local * lax.axis_size("band") * kpoint_local * lax.axis_size("grid")
    )
    cas_grid = cas_table(grid_size)
    shifted = shift_axis(potential, sites[0, 0], 0)
    shifted = shift_axis(shifted, sites[1, 0], 1)
    shifted = shift_axis(shifted, sites[2, 0], 2)
    tables = [shifted]
    shifted_all = jnp.stack(tables, axis=-1)
    slab_table = lax.dynamic_slice_in_dim(shifted_all, position * plane_count, plane_count, 1)

    def moment(left, right):
        return jnp.sum(left * right, axis=(1, 3, 4)) / total_count

    start_sum = lax.psum(moment(start, start), ("grid", "band"))
    lanczos = start / expand_coef(jnp.sqrt(start_sum))
    previous = jnp.zeros_like(start)
    beta_prev = jnp.zeros((atom_count, pol_count), jnp.float32)
    alpha_list = []
    beta_list = []
    for iteration in range(ITERS):
        spread_fields = lanczos.reshape(atom_count, chain_count, plane_count, grid_size, grid_size)
        spread_over_z = jnp.einsum(
            "arpyz,wz->pywar", spread_fields, cas_grid, precision=precise_mode
        )
        spread_over_y = jnp.einsum(
            "pywar,uy->puwar", spread_over_z, cas_grid, precision=precise_mode
        )
        direct_spectrum = lax.all_to_all(
            spread_over_y.reshape(plane_count, grid_size, grid_size, field_count),
            "grid",
            split_axis=1,
            concat_axis=0,
            tiled=True,
        )
        field_shape = direct_spectrum.shape
        over_x = jnp.einsum("xvwf,tx->tvwf", direct_spectrum, cas_grid, precision=precise_mode)
        split_view = over_x.reshape(
            field_shape[0], field_shape[1], field_shape[2], atom_count, chain_count
        )
        scaled = split_view * slab_table[..., None]
        back_x = jnp.einsum("tvwar,xt->xvwar", scaled, cas_grid, precision=precise_mode)
        weighted = back_x.reshape(field_shape)
        direct_returned = lax.all_to_all(weighted, "grid", split_axis=0, concat_axis=1, tiled=True)
        fields = direct_returned.reshape(plane_count, grid_size, grid_size, atom_count, chain_count)
        over_z = jnp.einsum("pvwar,zw->pvzar", fields, cas_grid, precision=precise_mode)
        over_y = jnp.einsum("pvzar,yv->arpyz", over_z, cas_grid, precision=precise_mode)
        applied = energies[None, :, None] * lanczos - over_y.reshape(start.shape) / volume
        moments_all = lax.psum(
            (
                moment(lanczos, applied),
                moment(applied, applied),
                moment(lanczos, lanczos),
                moment(previous, previous),
                moment(previous, applied),
                moment(lanczos, previous),
            ),
            ("grid", "band"),
        )
        alpha_now = moments_all[0]
        square = (
            moments_all[1]
            + alpha_now * alpha_now * moments_all[2]
            + beta_prev * beta_prev * moments_all[3]
        )
        square = square - 2.0 * alpha_now * moments_all[0] - 2.0 * beta_prev * moments_all[4]
        square = square + 2.0 * alpha_now * beta_prev * moments_all[5]
        beta_now = jnp.sqrt(square)
        remainder = applied - expand_coef(alpha_now) * lanczos - expand_coef(beta_prev) * previous
        previous = lanczos
        lanczos = remainder / expand_coef(beta_now)
        beta_prev = beta_now
        alpha_list.append(alpha_now)
        beta_list.append(beta_now)
    return (jnp.stack(alpha_list, axis=2), jnp.stack(beta_list, axis=2), lanczos)


MESH = pl.DeviceIdType.MESH
LANES = 128
SUBLANES = 8
GROUPS = 2
EARLY = 1
FIRST_EIGHTHS = 5
PART = SUBLANES // GROUPS


def split(value):
    high = value.astype(jnp.bfloat16)
    return high, (value - high.astype(jnp.float32)).astype(jnp.bfloat16)


def dot3(left, right):
    left_high, left_low = left
    right_high, right_low = right
    left = jnp.concatenate([left_high, left_low, left_high], axis=1)
    right = jnp.concatenate([right_high, right_high, right_low], axis=0)
    return jnp.dot(left, right, preferred_element_type=jnp.float32)


def shifted_potential(table, sites, grid_size):
    cells = grid_size * grid_size
    lane = lax.broadcasted_iota(jnp.int32, table.shape, 1) % grid_size
    for axis in range(3):
        step = 1
        while step < grid_size:
            if axis == 0:
                moved = pltpu.roll(table, step, 0)
            elif axis == 1:
                moved = pltpu.roll(table, step * grid_size, 1)
            else:
                moved = jnp.where(
                    lane >= step,
                    pltpu.roll(table, step, 1),
                    pltpu.roll(table, cells - grid_size + step, 1),
                )
            flag = jnp.full(table.shape, sites[axis] // step % 2, jnp.int32)
            table = jnp.where(flag == 1, moved, table)
            step *= 2
    return table


def total_of(parts):
    total = parts[0]
    for part in parts[1:]:
        total = total + part
    return jnp.sum(jnp.sum(total, axis=0, keepdims=True), axis=1, keepdims=True)


def inverse_of(value):
    return jnp.where(value > 0.0, 1.0 / jnp.where(value > 0.0, value, 1.0), 0.0)


def frequency_order(grid_size):
    cells = np.arange(grid_size)
    return np.concatenate([cells[0::4], cells[2::4], cells[1::2]])


def recursion_kernel(
    sizes, start, energies, sites, pot, forward_y, back_y, all_z, x_far,
    land, coef,
    sites_here, forward_y_here, back_y_here, all_z_here, x_wide, pot_here, pot_flat, pot_order,
    start_here, energy_here, packed, basis, energy, site_table,
    to_high, to_low, from_high, from_low, vec_high, vec_low, mid_high, mid_low, past,
    outgoing, early_land, sums, gathered,
    table_sem, load_sem, send_sem, recv_sem, out_send, out_recv, sum_send, sum_recv, plane_sem, early_send, early_recv,
):
    n, band_n, grid_size, halves = sizes
    me = lax.axis_index("grid")
    band = lax.axis_index("band")
    rank = band * n + me
    members = n * band_n
    cells = grid_size * grid_size
    planes = grid_size // n
    rows = grid_size * PART
    piece = planes * PART
    early = EARLY * piece // 2
    quarter = cells // 4
    total_count = float(grid_size * SUBLANES * cells * members)

    load_copies = [
        pltpu.make_async_copy(source, target, load_sem.at[i])
        for i, (source, target) in enumerate(((start, start_here), (energies, energy_here)))
    ]
    table_copies = [
        pltpu.make_async_copy(source, target, table_sem.at[i])
        for i, (source, target) in enumerate((
            (forward_y, forward_y_here), (back_y, back_y_here), (all_z, all_z_here), (x_far, x_wide), (pot, pot_here), (sites, sites_here)))
    ]
    for copy in load_copies + table_copies:
        copy.start()
    barrier = pltpu.get_barrier_semaphore()
    for k in range(1, band_n):
        pl.semaphore_signal(barrier, inc=1, device_id={"band": (band + k) % band_n}, device_id_type=MESH)
    for k in range(1, n):
        pl.semaphore_signal(barrier, inc=1, device_id={"grid": (me + k) % n}, device_id_type=MESH)

    upper = lax.broadcasted_iota(jnp.int32, (SUBLANES, cells), 0) < PART

    def pack(kind):
        def pack_owner(owner, carry):
            at = pl.ds(pl.multiple_of(owner % halves * SUBLANES, SUBLANES), SUBLANES)
            for pair in range(planes // 2):
                first, second = slice(2 * pair * cells, (2 * pair + 1) * cells), slice((2 * pair + 1) * cells, (2 * pair + 2) * cells)
                if kind == 0:
                    one, two = start_here[0, owner // halves, 0, at, first], start_here[0, owner // halves, 0, at, second]
                else:
                    one, two = energy_here[owner // halves, at, first], energy_here[owner // halves, at, second]
                here = slice(pair * SUBLANES, (pair + 1) * SUBLANES)
                packed[kind, 0, owner, here, :] = jnp.where(upper, one, pltpu.roll(two, PART, 0))
                packed[kind, 1, owner, here, :] = jnp.where(upper, pltpu.roll(one, PART, 0), two)
            return carry

        lax.fori_loop(0, n, pack_owner, 0)

    my_rows = pl.ds(pl.multiple_of(me * piece, piece), piece)

    def piece_copy(kind, group, k):
        peer = (me + k) % n
        target = basis.at[group, 0, my_rows, :] if kind == 0 else energy.at[group, my_rows, :]
        return pltpu.make_async_remote_copy(
            src_ref=packed.at[kind, group, peer], dst_ref=target, send_sem=send_sem.at[kind, group, k],
            recv_sem=recv_sem.at[kind, group, k], device_id={"grid": peer}, device_id_type=MESH)

    load_copies[0].wait()
    pack(0)
    load_copies[1].wait()
    pack(1)
    pl.semaphore_wait(barrier, n + band_n - 2)
    for group in range(GROUPS):
        for kind in range(2):
            for k in range(1, n):
                piece_copy(kind, group, k).start()
    for k in range(1, band_n):
        pl.semaphore_signal(plane_sem, inc=1, device_id={"band": (band + k) % band_n}, device_id_type=MESH)
    for group in range(GROUPS):
        basis[group, 0, my_rows, :] = packed[0, group, me]
        energy[group, my_rows, :] = packed[1, group, me]

    for copy in table_copies:
        copy.wait()

    def forward_rows(y, carry):
        high, low = split(forward_y_here[pl.ds(y, 1), :] * all_z_here[...])
        at = pl.ds(pl.multiple_of(y * grid_size, grid_size), grid_size)
        to_high[at, :] = high
        to_low[at, :] = low
        return carry

    def back_rows(v, carry):
        high, low = split(back_y_here[pl.ds(v, 1), :] * all_z_here[:, : 2 * quarter])
        at = pl.ds(pl.multiple_of(v * grid_size, grid_size), grid_size)
        from_high[at, :] = high
        from_low[at, :] = low
        return carry

    lax.fori_loop(0, grid_size // 2, forward_rows, 0)
    lax.fori_loop(0, grid_size, back_rows, 0)
    for y in range(grid_size):
        pot_flat[:, y * grid_size:(y + 1) * grid_size] = pot_here[:, y, :]
    pot_flat[...] = shifted_potential(pot_flat[...], sites_here, grid_size) * (1.0 / (grid_size * cells))
    for place, v in enumerate(frequency_order(grid_size)):
        pot_order[:, place * grid_size:(place + 1) * grid_size] = pot_flat[:, int(v) * grid_size:(int(v) + 1) * grid_size]
    for x in range(grid_size):
        site_table[PART * x:PART * (x + 1), :] = jnp.broadcast_to(pot_order[x:x + 1, :], (PART, cells))

    past[...] = jnp.zeros_like(past)
    pl.semaphore_wait(plane_sem, band_n - 1)

    quarters = [slice(i * quarter, (i + 1) * quarter) for i in range(4)]
    odd = slice(2 * quarter, 4 * quarter)
    lane = lax.broadcasted_iota(jnp.int32, (1, LANES), 1)
    tall = 2 * SUBLANES

    def lane_is(place):
        return lane == jnp.full((1, LANES), place, jnp.int32)

    def folded(product):
        return sum((product[i:i + SUBLANES] for i in range(SUBLANES, product.shape[0], SUBLANES)), product[:SUBLANES])

    def times_x(value):
        high, low = split(value)
        return jnp.dot(x_wide[...], jnp.concatenate([high, high, low], axis=0), preferred_element_type=jnp.float32)

    first_columns = cells * FIRST_EIGHTHS // 8
    early_columns = (pl.ds(0, first_columns), pl.ds(first_columns, cells - first_columns))

    def early_copy(part, k):
        peer = (me + k) % n
        at = pl.ds(pl.multiple_of(peer * piece, SUBLANES), early)
        return pltpu.make_async_remote_copy(
            src_ref=basis.at[0, pl.ds(1, ITERS), at, early_columns[part]], dst_ref=early_land.at[me, :, :, early_columns[part]],
            send_sem=early_send.at[part, k], recv_sem=early_recv.at[part, k], device_id={"grid": peer}, device_id_type=MESH)

    def message_copy(stage, k):
        return pltpu.make_async_remote_copy(
            src_ref=sums.at[stage, rank], dst_ref=sums.at[stage, rank], send_sem=sum_send.at[stage, k], recv_sem=sum_recv.at[stage, k],
            device_id={"grid": (me + k % n) % n, "band": (band + k // n) % band_n}, device_id_type=MESH)

    far_first = sorted(range(1, members), key=lambda k: -min(k // n, band_n - k // n))

    def send_message(stage, message):
        sums[stage, rank] = message
        for k in far_first:
            message_copy(stage, k).start()

    tiles = [slice(r, r + tall) for r in range(0, rows, tall)]

    def spread_quarters(at, q):
        even, other = q[0] + q[2], q[1] + q[3]
        for cols, value in zip(quarters, (even + other, even - other, q[0] - q[2], q[1] - q[3])):
            vec_high[at, cols], vec_low[at, cols] = split(value)

    def settle(t, results):
        alpha_part, square_part, norm, norm_before, message = results
        j = (t + ITERS - 1) % ITERS
        alpha = total_of([alpha_part]) * inverse_of(norm)
        gamma = jnp.where(jnp.full((1, 1), j, jnp.int32) == 0, 0.0, norm * inverse_of(norm_before))
        norm_after = jnp.maximum(total_of([square_part]) - alpha * alpha * norm - gamma * norm, 0.0)
        place = SUBLANES * ((t + ITERS - 1) // ITERS - 1) + j
        message = jnp.where(lane_is(place), norm, message)
        message = jnp.where(lane_is(place + 1), norm_after, message)
        message = jnp.where(lane_is(place + LANES // 2), alpha, message)
        return alpha, gamma, message

    def step(t, results, final=False):
        alpha, gamma, message = settle(t, results)
        group, j = t // ITERS, t % ITERS
        before, earlier, now = jnp.maximum(j - 1, 0), jnp.maximum(j - 2, 0), j % 2
        if final:
            send_message(0, message)
        else:
            keep = jnp.where(jnp.full((1, 1), j, jnp.int32) == 0, 0.0, 1.0)
            alpha, gamma = alpha * keep, gamma * keep

            @pl.when(j == 0)
            def _():
                for k in range(1, n):
                    piece_copy(0, group, k).wait_recv()
                for at in tiles:
                    spread_quarters(at, [basis[group, 0, at, cols] for cols in quarters])

        def forward(i):
            cols = quarters[i]
            source, depth = (cols, quarter) if i < 2 else (odd, 2 * quarter)
            spectrum = dot3((vec_high[:, source], vec_low[:, source]), (to_high[:depth, cols], to_low[:depth, cols]))
            spectrum = spectrum - alpha * past[1 - now, :, cols] - gamma * past[now, :, cols]
            past[now, :, cols] = spectrum
            return spectrum

        def weigh(i, spectrum):
            return times_x(spectrum) * site_table[:, quarters[i]]

        def finish(i, spectrum):
            mid_high[:, quarters[i]], mid_low[:, quarters[i]] = split(times_x(spectrum))

        first, second = forward(0), forward(1)
        first = weigh(0, first)
        third = forward(2)
        second = weigh(1, second)
        finish(0, first)
        fourth = forward(3)
        third = weigh(2, third)
        finish(1, second)
        fourth = weigh(3, fourth)
        finish(2, third)
        finish(3, fourth)
        norm_part = jnp.zeros((SUBLANES, quarter), jnp.float32)
        for at in tiles:
            for cols in quarters:
                value = basis[group, j, at, cols] - alpha * basis[group, before, at, cols] - gamma * basis[group, earlier, at, cols]
                basis[group, j, at, cols] = value
                norm_part = norm_part + folded(value * value)
        norm = total_of([norm_part])
        if not final:

            @pl.when(j == 0)
            def _():
                for k in range(1, n):
                    piece_copy(1, group, k).wait_recv()

            @pl.when(t == ITERS)
            def _():
                for k in range(1, n):
                    early_copy(0, k).start()

        def back(at, cols):
            return dot3((mid_high[:, at], mid_low[:, at]), (from_high[at, cols], from_low[at, cols]))

        zero, two = back(quarters[0], slice(0, quarter)), back(quarters[1], slice(0, quarter))
        odds = back(odd, slice(0, 2 * quarter))
        alpha_part, square_part = jnp.zeros((SUBLANES, quarter), jnp.float32), jnp.zeros((SUBLANES, quarter), jnp.float32)
        for at in tiles:
            plus, minus, one, three = zero[at] + two[at], zero[at] - two[at], odds[at, :quarter], odds[at, quarter:]
            q = []
            for cols, value in zip(quarters, (plus + one, minus + three, plus - one, minus - three)):
                here = basis[group, j, at, cols]
                new = energy[group, at, cols] * here - value
                basis[group, j + 1, at, cols] = new
                alpha_part = alpha_part + folded(here * new)
                square_part = square_part + folded(new * new)
                q.append(new)
            if not final:
                spread_quarters(at, q)
        return alpha_part, square_part, norm, results[2], message

    nothing, no_part = jnp.zeros((1, 1), jnp.float32), jnp.zeros((SUBLANES, quarter), jnp.float32)
    results = (no_part, no_part, nothing, nothing, jnp.zeros((1, LANES), jnp.float32))
    steps = GROUPS * ITERS
    results = step(steps - 1, lax.fori_loop(0, steps - 1, step, results), True)
    send_message(1, settle(steps, results)[2])
    for k in range(1, n):
        early_copy(1, k).start()

    def tables_of(stage):
        for k in range(1, members):
            message_copy(stage, k).wait_recv()
        for r in range(members):
            gathered[stage, r:r + 1, :] = sums[stage, r]
        table = gathered[stage]
        norms = jnp.where(wide_lane < LANES // 2, table, 0.0)
        return norms, pltpu.roll(table, LANES // 2, 1), jnp.where(order > 0, norms * inverse_of(pltpu.roll(norms, 1, 1)), 0.0)

    wide_lane = lax.broadcasted_iota(jnp.int32, (members, LANES), 1)
    order = wide_lane % SUBLANES
    used = jnp.logical_and(order <= ITERS, wide_lane < SUBLANES * GROUPS)

    def inner(norms, left, right):
        return total_of([norms * left * right]) / total_count

    def global_step(tables, vector, previous, beta):
        norms, diagonal, coupling = tables
        raised = jnp.where(order > 0, pltpu.roll(vector, 1, 1), 0.0)
        lowered = jnp.where(order < ITERS, pltpu.roll(coupling * vector, LANES - 1, 1), 0.0)
        image = jnp.where(used, raised + jnp.where(order < ITERS, diagonal, 0.0) * vector + lowered, 0.0)
        alpha_now = inner(norms, vector, image)
        rest = image - alpha_now * vector - beta * previous
        beta_now = jnp.sqrt(inner(norms, rest, rest))
        return alpha_now, beta_now, rest / beta_now, vector

    alphas, betas = jnp.zeros((1, LANES), jnp.float32), jnp.zeros((1, LANES), jnp.float32)
    tables = tables_of(0)
    first = jnp.where(jnp.logical_and(used, order == 0), 1.0, 0.0)
    vector, previous, beta = first / jnp.sqrt(inner(tables[0], first, first)), jnp.zeros((members, LANES), jnp.float32), nothing
    for j in range(ITERS):
        if j == ITERS - 1:
            tables = tables_of(1)
        alpha, beta, vector, previous = global_step(tables, vector, previous, beta)
        alphas, betas = jnp.where(lane == j, alpha, alphas), jnp.where(lane == j, beta, betas)
    coef[0:1, :] = alphas
    coef[1:2, :] = betas
    norms, diagonal, coupling = tables
    top = ITERS - 1
    weights = vector - jnp.where(order == top, diagonal * pltpu.roll(vector, LANES - 1, 1), 0.0)
    weights = weights - jnp.where(order == top - 1, pltpu.roll(coupling, LANES - 1, 1) * pltpu.roll(vector, LANES - 2, 1), 0.0)
    gathered[2] = weights

    def scales_of(owner):
        row = gathered[2, pl.ds(owner, 1), :]
        return [
            [jnp.sum(jnp.where(lane == SUBLANES * group + i, row, 0.0), axis=1, keepdims=True) for i in range(ITERS + 1)]
            for group in range(GROUPS)
        ]

    scales = scales_of(rank)
    out_copies = []
    for k in range(1, n + 1):
        peer = (me + k) % n
        for group in range(GROUPS):
            skip = early if group == 0 and k < n else 0
            at = pl.ds(pl.multiple_of(peer * piece + skip, SUBLANES), piece - skip)
            value = sum((scales[group][i] * basis[group, i, at, :] for i in range(1, ITERS + 1)), scales[group][0] * basis[group, 0, at, :])
            target = slice(group * piece + skip, (group + 1) * piece)
            if k < n:
                outgoing[peer, target, :] = value
            else:
                land[me, target, :] = value
        if k < n:
            sent = pl.ds(early, GROUPS * piece - early)
            copy = pltpu.make_async_remote_copy(
                src_ref=outgoing.at[peer, sent, :], dst_ref=land.at[me, sent, :], send_sem=out_send.at[k], recv_sem=out_recv.at[k],
                device_id={"grid": peer}, device_id_type=MESH)
            copy.start()
            out_copies.append(copy)
    for k in range(1, n):
        for part in range(2):
            early_copy(part, k).wait()
        peer = (me + n - k) % n
        scale = scales_of(band * n + peer)[0]
        value = scale[0] * packed[0, 0, peer, :early, :]
        for i in range(1, ITERS + 1):
            value = value + scale[i] * early_land[peer, i - 1]
        land[peer, :early, :] = value
    for group in range(GROUPS):
        for kind in range(2):
            for k in range(1, n):
                piece_copy(kind, group, k).wait_send()
    for stage in range(2):
        for k in range(1, members):
            message_copy(stage, k).wait_send()
    for copy in out_copies:
        copy.wait()


def unpack_kernel(halves, planes, land, coef, out, alphas, betas):
    owners, cells = land.shape[0], land.shape[2]
    upper = lax.broadcasted_iota(jnp.int32, (SUBLANES, cells), 0) < PART
    for owner in range(owners):
        at = slice(owner % halves * SUBLANES, (owner % halves + 1) * SUBLANES)
        for pair in range(planes // 2):
            here = slice(pair * SUBLANES, (pair + 1) * SUBLANES)
            one, two = land[owner, here, :], land[owner, slice(here.start + planes * PART, here.stop + planes * PART), :]
            out[0, owner // halves, 0, at, 2 * pair * cells:(2 * pair + 1) * cells] = jnp.where(upper, one, pltpu.roll(two, PART, 0))
            out[0, owner // halves, 0, at, (2 * pair + 1) * cells:(2 * pair + 2) * cells] = jnp.where(upper, pltpu.roll(one, PART, 0), two)
    alphas[0] = coef[0:1, :ITERS]
    betas[0] = coef[1:2, :ITERS]


def field_body(start, energies, sites, potential):
    grid_size = potential.shape[0]
    cells = grid_size * grid_size
    n, band_n = lax.axis_size("grid"), lax.axis_size("band")
    halves = start.shape[3] // SUBLANES
    planes = grid_size // n
    rows, piece, half_cells = grid_size * PART, planes * PART, cells // 2
    index = np.arange(grid_size)
    angle = (index[:, None] * index[None, :] % grid_size) * (2.0 * math.pi / grid_size)
    cas = np.cos(angle) + np.sin(angle)
    ordered = cas[frequency_order(grid_size)]
    half_grid = grid_size // 2
    forward_y = jnp.asarray(np.repeat(ordered.T[:half_grid], grid_size, axis=1), jnp.float32)
    back_y = jnp.asarray(np.repeat(ordered[:, :half_grid], grid_size, axis=1), jnp.float32)
    all_z = jnp.asarray(np.tile(cas, (1, grid_size)), jnp.float32)
    x_wide = np.kron(cas, np.eye(PART)).astype(np.float32)
    x_high = x_wide.astype(jnp.bfloat16)
    x_low = (x_wide - x_high.astype(np.float32)).astype(jnp.bfloat16)
    x_wide = jnp.asarray(np.concatenate([x_high, x_low, x_high], axis=1))
    vmem = pl.BlockSpec(memory_space=pltpu.VMEM)
    hbm = pl.BlockSpec(memory_space=pltpu.MemorySpace.HBM)
    f32, bf16 = jnp.float32, jnp.bfloat16
    dma = pltpu.SemaphoreType.DMA
    members = n * band_n
    land_shape = (n, GROUPS * piece, cells)
    operands = (start, energies, sites[:, 0], potential, forward_y, back_y, all_z, x_wide)
    operands = (pltpu.with_memory_space_constraint(value, pltpu.MemorySpace.HBM) for value in operands)
    land, coef = pl.pallas_call(
        functools.partial(recursion_kernel, (n, band_n, grid_size, halves)),
        out_shape=(jax.ShapeDtypeStruct(land_shape, f32), jax.ShapeDtypeStruct((2, LANES), f32)),
        in_specs=[hbm] * 8,
        out_specs=(vmem, vmem),
        scratch_shapes=[
            pltpu.SMEM((3,), jnp.int32),
            pltpu.VMEM((half_grid, cells), f32), pltpu.VMEM((grid_size, half_cells), f32), pltpu.VMEM((grid_size, cells), f32),
            pltpu.VMEM((rows, 3 * rows), bf16), pltpu.VMEM(potential.shape, f32),
            pltpu.VMEM((grid_size, cells), f32), pltpu.VMEM((grid_size, cells), f32),
            pltpu.VMEM(start.shape, f32), pltpu.VMEM(energies.shape, f32),
            pltpu.VMEM((2, GROUPS, n, piece, cells), f32),
            pltpu.VMEM((GROUPS, ITERS + 1, rows, cells), f32), pltpu.VMEM((GROUPS, rows, cells), f32),
            pltpu.VMEM((rows, cells), f32),
            pltpu.VMEM((half_cells, cells), bf16), pltpu.VMEM((half_cells, cells), bf16),
            pltpu.VMEM((cells, half_cells), bf16), pltpu.VMEM((cells, half_cells), bf16),
            pltpu.VMEM((rows, cells), bf16), pltpu.VMEM((rows, cells), bf16),
            pltpu.VMEM((rows, cells), bf16), pltpu.VMEM((rows, cells), bf16),
            pltpu.VMEM((2, rows, cells), f32), pltpu.VMEM(land_shape, f32),
            pltpu.VMEM((n, ITERS, EARLY * piece // 2, cells), f32),
            pltpu.VMEM((2, members, 1, LANES), f32), pltpu.VMEM((3, members, LANES), f32),
            dma((6,)), dma((2,)), dma((2, GROUPS, n)), dma((2, GROUPS, n)), dma((n,)), dma((n,)),
            dma((2, members)), dma((2, members)), pltpu.SemaphoreType.REGULAR, dma((2, n)), dma((2, n)),
        ],
        compiler_params=pltpu.CompilerParams(collective_id=0, has_side_effects=True, vmem_limit_bytes=36 * 1024 * 1024),
    )(*operands)
    scalar = jax.ShapeDtypeStruct((1, 1, ITERS), f32)
    out, alphas, betas = pl.pallas_call(
        functools.partial(unpack_kernel, halves, planes),
        out_shape=(jax.ShapeDtypeStruct(start.shape, f32), scalar, scalar),
        in_specs=[vmem, vmem],
        out_specs=(vmem, vmem, vmem),
        compiler_params=pltpu.CompilerParams(vmem_limit_bytes=8 * 1024 * 1024),
    )(land, coef)
    return alphas, betas, out


def body(start, energies, sites, potential):
    atoms, cores, pols, bands, _ = start.shape
    grid_size = potential.shape[0]
    n = lax.axis_size("grid")
    whole_fields = (
        atoms == 1 and pols == 1 and bands % SUBLANES == 0 and cores * bands == SUBLANES * n
        and grid_size % (2 * SUBLANES) == 0 and grid_size % (2 * n) == 0
        and grid_size * grid_size % (4 * LANES) == 0 and n * lax.axis_size("band") % SUBLANES == 0
    )
    return (field_body if whole_fields else plane_body)(start, energies, sites, potential)


def solution(mesh):
    in_specs = (P(None, None, None, "band", "grid"), P(None, "band", "grid"), P(), P())
    out_specs = (P(), P(), P(None, None, None, "band", "grid"))
    return jax.shard_map(body, mesh=mesh, in_specs=in_specs, out_specs=out_specs, check_vma=False)
```

```python
import functools
import math

import jax
import jax.numpy as jnp
import numpy as np
from jax import lax
from jax.experimental import pallas as pl
from jax.experimental.pallas import tpu as pltpu
from jax.sharding import PartitionSpec as P

ITERS = 4


precise_mode = lax.Precision.HIGHEST


def cas_table(grid_size):
    cells = jnp.arange(grid_size, dtype=jnp.int32)
    phase = cells[:, None] * cells[None, :] % grid_size
    angle = phase.astype(jnp.float32) * (2.0 * math.pi / grid_size)
    return jnp.cos(angle) + jnp.sin(angle)


def shift_axis(field_part, offset, axis_number):
    length = field_part.shape[axis_number]
    doubled = jnp.concatenate([field_part, field_part], axis=axis_number)
    first_index = (length - offset) % length
    return lax.dynamic_slice_in_dim(doubled, first_index, length, axis_number)


def expand_coef(values):
    return values[:, None, :, None, None]


def plane_body(start, energies, sites, potential):
    grid_size = potential.shape[0]
    volume = grid_size * grid_size * grid_size
    atom_count, core_count, pol_count, band_local, kpoint_local = start.shape
    plane_count = grid_size // lax.axis_size("grid")
    position = lax.axis_index("grid")
    chain_count = core_count * pol_count * band_local
    field_count = atom_count * chain_count
    total_count = (
        core_count * band_local * lax.axis_size("band") * kpoint_local * lax.axis_size("grid")
    )
    cas_grid = cas_table(grid_size)
    shifted = shift_axis(potential, sites[0, 0], 0)
    shifted = shift_axis(shifted, sites[1, 0], 1)
    shifted = shift_axis(shifted, sites[2, 0], 2)
    tables = [shifted]
    shifted_all = jnp.stack(tables, axis=-1)
    slab_table = lax.dynamic_slice_in_dim(shifted_all, position * plane_count, plane_count, 1)

    def moment(left, right):
        return jnp.sum(left * right, axis=(1, 3, 4)) / total_count

    start_sum = lax.psum(moment(start, start), ("grid", "band"))
    lanczos = start / expand_coef(jnp.sqrt(start_sum))
    previous = jnp.zeros_like(start)
    beta_prev = jnp.zeros((atom_count, pol_count), jnp.float32)
    alpha_list = []
    beta_list = []
    for iteration in range(ITERS):
        spread_fields = lanczos.reshape(atom_count, chain_count, plane_count, grid_size, grid_size)
        spread_over_z = jnp.einsum(
            "arpyz,wz->pywar", spread_fields, cas_grid, precision=precise_mode
        )
        spread_over_y = jnp.einsum(
            "pywar,uy->puwar", spread_over_z, cas_grid, precision=precise_mode
        )
        direct_spectrum = lax.all_to_all(
            spread_over_y.reshape(plane_count, grid_size, grid_size, field_count),
            "grid",
            split_axis=1,
            concat_axis=0,
            tiled=True,
        )
        field_shape = direct_spectrum.shape
        over_x = jnp.einsum("xvwf,tx->tvwf", direct_spectrum, cas_grid, precision=precise_mode)
        split_view = over_x.reshape(
            field_shape[0], field_shape[1], field_shape[2], atom_count, chain_count
        )
        scaled = split_view * slab_table[..., None]
        back_x = jnp.einsum("tvwar,xt->xvwar", scaled, cas_grid, precision=precise_mode)
        weighted = back_x.reshape(field_shape)
        direct_returned = lax.all_to_all(weighted, "grid", split_axis=0, concat_axis=1, tiled=True)
        fields = direct_returned.reshape(plane_count, grid_size, grid_size, atom_count, chain_count)
        over_z = jnp.einsum("pvwar,zw->pvzar", fields, cas_grid, precision=precise_mode)
        over_y = jnp.einsum("pvzar,yv->arpyz", over_z, cas_grid, precision=precise_mode)
        applied = energies[None, :, None] * lanczos - over_y.reshape(start.shape) / volume
        moments_all = lax.psum(
            (
                moment(lanczos, applied),
                moment(applied, applied),
                moment(lanczos, lanczos),
                moment(previous, previous),
                moment(previous, applied),
                moment(lanczos, previous),
            ),
            ("grid", "band"),
        )
        alpha_now = moments_all[0]
        square = (
            moments_all[1]
            + alpha_now * alpha_now * moments_all[2]
            + beta_prev * beta_prev * moments_all[3]
        )
        square = square - 2.0 * alpha_now * moments_all[0] - 2.0 * beta_prev * moments_all[4]
        square = square + 2.0 * alpha_now * beta_prev * moments_all[5]
        beta_now = jnp.sqrt(square)
        remainder = applied - expand_coef(alpha_now) * lanczos - expand_coef(beta_prev) * previous
        previous = lanczos
        lanczos = remainder / expand_coef(beta_now)
        beta_prev = beta_now
        alpha_list.append(alpha_now)
        beta_list.append(beta_now)
    return (jnp.stack(alpha_list, axis=2), jnp.stack(beta_list, axis=2), lanczos)


MESH = pl.DeviceIdType.MESH
LANES = 128
SUBLANES = 8
GROUPS = 2
EARLY_EIGHTHS = (4, 3)
ORDER = "F0 F1 F2 F3 W0 W1 W2 W3 X0 X1 X2 X3"
PART = SUBLANES // GROUPS


def split(value):
    high = value.astype(jnp.bfloat16)
    return high, (value - high.astype(jnp.float32)).astype(jnp.bfloat16)


def dot3(left, right):
    left_high, left_low = left
    right_high, right_low = right
    left = jnp.concatenate([left_high, left_low, left_high], axis=1)
    right = jnp.concatenate([right_high, right_high, right_low], axis=0)
    return jnp.dot(left, right, preferred_element_type=jnp.float32)


def shifted_potential(table, sites, grid_size):
    cells = grid_size * grid_size
    lane = lax.broadcasted_iota(jnp.int32, table.shape, 1) % grid_size
    for axis in range(3):
        step = 1
        while step < grid_size:
            if axis == 0:
                moved = pltpu.roll(table, step, 0)
            elif axis == 1:
                moved = pltpu.roll(table, step * grid_size, 1)
            else:
                moved = jnp.where(
                    lane >= step,
                    pltpu.roll(table, step, 1),
                    pltpu.roll(table, cells - grid_size + step, 1),
                )
            flag = jnp.full(table.shape, sites[axis] // step % 2, jnp.int32)
            table = jnp.where(flag == 1, moved, table)
            step *= 2
    return table


def total_of(parts):
    total = parts[0]
    for part in parts[1:]:
        total = total + part
    return jnp.sum(jnp.sum(total, axis=0, keepdims=True), axis=1, keepdims=True)


def inverse_of(value):
    return jnp.where(value > 0.0, 1.0 / jnp.where(value > 0.0, value, 1.0), 0.0)


def frequency_order(grid_size):
    cells = np.arange(grid_size)
    return np.concatenate([cells[0::4], cells[2::4], cells[1::2]])


def recursion_kernel(
    sizes, start, energies, sites, pot, forward_y, back_y, all_z, x_far,
    land, coef,
    sites_here, forward_y_here, back_y_here, all_z_here, x_wide, pot_here, pot_flat, pot_order,
    start_here, energy_here, packed, basis, energy, site_table,
    to_high, to_low, from_high, from_low, vec_high, vec_low, mid_high, mid_low, past,
    outgoing, early_land, sums, gathered,
    table_sem, load_sem, send_sem, recv_sem, out_send, out_recv, sum_send, sum_recv, plane_sem, early_send, early_recv,
):
    n, band_n, grid_size, halves = sizes
    me = lax.axis_index("grid")
    band = lax.axis_index("band")
    rank = band * n + me
    members = n * band_n
    cells = grid_size * grid_size
    planes = grid_size // n
    rows = grid_size * PART
    piece = planes * PART
    early = piece // 2
    quarter = cells // 4
    total_count = float(grid_size * SUBLANES * cells * members)

    load_copies = [
        pltpu.make_async_copy(source, target, load_sem.at[i])
        for i, (source, target) in enumerate(((start, start_here), (energies, energy_here)))
    ]
    table_copies = [
        pltpu.make_async_copy(source, target, table_sem.at[i])
        for i, (source, target) in enumerate((
            (forward_y, forward_y_here), (back_y, back_y_here), (all_z, all_z_here), (x_far, x_wide), (pot, pot_here), (sites, sites_here)))
    ]
    load_copies[0].start()
    barrier = pltpu.get_barrier_semaphore()
    for k in range(1, band_n):
        pl.semaphore_signal(barrier, inc=1, device_id={"band": (band + k) % band_n}, device_id_type=MESH)
    for k in range(1, n):
        pl.semaphore_signal(barrier, inc=1, device_id={"grid": (me + k) % n}, device_id_type=MESH)

    upper = lax.broadcasted_iota(jnp.int32, (SUBLANES, cells), 0) < PART

    def pack(kind):
        def pack_owner(owner, carry):
            at = pl.ds(pl.multiple_of(owner % halves * SUBLANES, SUBLANES), SUBLANES)
            for pair in range(planes // 2):
                first, second = slice(2 * pair * cells, (2 * pair + 1) * cells), slice((2 * pair + 1) * cells, (2 * pair + 2) * cells)
                if kind == 0:
                    one, two = start_here[0, owner // halves, 0, at, first], start_here[0, owner // halves, 0, at, second]
                else:
                    one, two = energy_here[owner // halves, at, first], energy_here[owner // halves, at, second]
                here = slice(pair * SUBLANES, (pair + 1) * SUBLANES)
                packed[kind, 0, owner, here, :] = jnp.where(upper, one, pltpu.roll(two, PART, 0))
                packed[kind, 1, owner, here, :] = jnp.where(upper, pltpu.roll(one, PART, 0), two)
            return carry

        lax.fori_loop(0, n, pack_owner, 0)

    my_rows = pl.ds(pl.multiple_of(me * piece, piece), piece)

    def piece_copy(kind, group, k):
        peer = (me + k) % n
        target = basis.at[group, 0, my_rows, :] if kind == 0 else energy.at[group, my_rows, :]
        return pltpu.make_async_remote_copy(
            src_ref=packed.at[kind, group, peer], dst_ref=target, send_sem=send_sem.at[kind, group, k],
            recv_sem=recv_sem.at[kind, group, k], device_id={"grid": peer}, device_id_type=MESH)

    load_copies[0].wait()
    for copy in load_copies[1:] + table_copies:
        copy.start()
    pack(0)
    pl.semaphore_wait(barrier, n + band_n - 2)
    for k in range(1, n):
        piece_copy(0, 0, k).start()
    load_copies[1].wait()
    pack(1)
    for kind, group in ((1, 0), (0, 1), (1, 1)):
        for k in range(1, n):
            piece_copy(kind, group, k).start()
    for k in range(1, band_n):
        pl.semaphore_signal(plane_sem, inc=1, device_id={"band": (band + k) % band_n}, device_id_type=MESH)
    for group in range(GROUPS):
        basis[group, 0, my_rows, :] = packed[0, group, me]
        energy[group, my_rows, :] = packed[1, group, me]

    for copy in table_copies:
        copy.wait()

    def forward_rows(y, carry):
        high, low = split(forward_y_here[pl.ds(y, 1), :] * all_z_here[...])
        at = pl.ds(pl.multiple_of(y * grid_size, grid_size), grid_size)
        to_high[at, :] = high
        to_low[at, :] = low
        return carry

    def back_rows(v, carry):
        high, low = split(back_y_here[pl.ds(v, 1), :] * all_z_here[:, : 2 * quarter])
        at = pl.ds(pl.multiple_of(v * grid_size, grid_size), grid_size)
        from_high[at, :] = high
        from_low[at, :] = low
        return carry

    lax.fori_loop(0, grid_size // 2, forward_rows, 0)
    lax.fori_loop(0, grid_size, back_rows, 0)
    for y in range(grid_size):
        pot_flat[:, y * grid_size:(y + 1) * grid_size] = pot_here[:, y, :]
    pot_flat[...] = shifted_potential(pot_flat[...], sites_here, grid_size) * (1.0 / (grid_size * cells))
    for place, v in enumerate(frequency_order(grid_size)):
        pot_order[:, place * grid_size:(place + 1) * grid_size] = pot_flat[:, int(v) * grid_size:(int(v) + 1) * grid_size]
    for x in range(grid_size):
        site_table[PART * x:PART * (x + 1), :] = jnp.broadcast_to(pot_order[x:x + 1, :], (PART, cells))

    pl.semaphore_wait(plane_sem, band_n - 1)

    quarters = [slice(i * quarter, (i + 1) * quarter) for i in range(4)]
    odd = slice(2 * quarter, 4 * quarter)
    lane = lax.broadcasted_iota(jnp.int32, (1, LANES), 1)
    tall = 2 * SUBLANES

    def lane_is(place):
        return lane == jnp.full((1, LANES), place, jnp.int32)

    def folded(product):
        return sum((product[i:i + SUBLANES] for i in range(SUBLANES, product.shape[0], SUBLANES)), product[:SUBLANES])

    def times_x(value):
        high, low = split(value)
        return jnp.dot(x_wide[...], jnp.concatenate([high, high, low], axis=0), preferred_element_type=jnp.float32)

    eighth = cells // 8
    early_columns = [pl.ds(sum(EARLY_EIGHTHS[:i]) * eighth, EARLY_EIGHTHS[i] * eighth) for i in range(len(EARLY_EIGHTHS))]
    early_stop = sum(EARLY_EIGHTHS) * eighth

    def early_copy(part, k):
        peer = (me + k) % n
        at = pl.ds(pl.multiple_of(peer * piece, SUBLANES), early)
        return pltpu.make_async_remote_copy(
            src_ref=basis.at[0, pl.ds(1, ITERS), at, early_columns[part]], dst_ref=early_land.at[me, :, :, early_columns[part]],
            send_sem=early_send.at[part, k], recv_sem=early_recv.at[part, k], device_id={"grid": peer}, device_id_type=MESH)

    def send_early(part):
        for k in range(1, n):
            early_copy(part, k).start()

    def message_copy(stage, k):
        return pltpu.make_async_remote_copy(
            src_ref=sums.at[stage, rank], dst_ref=sums.at[stage, rank], send_sem=sum_send.at[stage, k], recv_sem=sum_recv.at[stage, k],
            device_id={"grid": (me + k % n) % n, "band": (band + k // n) % band_n}, device_id_type=MESH)

    far_first = sorted(range(1, members), key=lambda k: -min(k // n, band_n - k // n))

    def send_message(stage, message):
        sums[stage, rank] = message
        for k in far_first:
            message_copy(stage, k).start()

    tiles = [slice(r, r + tall) for r in range(0, rows, tall)]

    def spread_quarters(at, q):
        even, other = q[0] + q[2], q[1] + q[3]
        for cols, value in zip(quarters, (even + other, even - other, q[0] - q[2], q[1] - q[3])):
            vec_high[at, cols], vec_low[at, cols] = split(value)

    def settle(t, results):
        alpha_part, square_part, norm, norm_before, message = results
        j = (t + ITERS - 1) % ITERS
        alpha = total_of([alpha_part]) * inverse_of(norm)
        gamma = jnp.where(jnp.full((1, 1), j, jnp.int32) == 0, 0.0, norm * inverse_of(norm_before))
        norm_after = jnp.maximum(total_of([square_part]) - alpha * alpha * norm - gamma * norm, 0.0)
        place = SUBLANES * ((t + ITERS - 1) // ITERS - 1) + j
        message = jnp.where(lane_is(place), norm, message)
        message = jnp.where(lane_is(place + 1), norm_after, message)
        message = jnp.where(lane_is(place + LANES // 2), alpha, message)
        return alpha, gamma, message

    def step(t, results, first=False, final=False):
        alpha, gamma, message = settle(t, results)
        group, j = t // ITERS, t % ITERS
        if final:
            send_message(0, message)
        if first:
            for k in range(1, n):
                piece_copy(0, group, k).wait_recv()
            for at in tiles:
                spread_quarters(at, [basis[group, 0, at, cols] for cols in quarters])
        else:
            before, earlier, now = j - 1, jnp.maximum(j - 2, 0), j % 2

        def forward(i):
            cols = quarters[i]
            source, depth = (cols, quarter) if i < 2 else (odd, 2 * quarter)
            spectrum = dot3((vec_high[:, source], vec_low[:, source]), (to_high[:depth, cols], to_low[:depth, cols]))
            if first:
                past[0, :, cols] = spectrum
                past[1, :, cols] = jnp.zeros_like(spectrum)
            else:
                spectrum = spectrum - alpha * past[1 - now, :, cols] - gamma * past[now, :, cols]
                past[now, :, cols] = spectrum
            return spectrum

        def weigh(i, spectrum):
            return times_x(past[0 if first else now, :, quarters[i]]) * site_table[:, quarters[i]]

        def finish(i, spectrum):
            mid_high[:, quarters[i]], mid_low[:, quarters[i]] = split(times_x(spectrum))

        work = {}
        for name in ORDER.split():
            i = int(name[1])
            if name[0] == "F":
                work[i] = forward(i)
            elif name[0] == "W":
                work[i] = weigh(i, work[i])
            else:
                finish(i, work[i])
        norm_part = jnp.zeros((SUBLANES, quarter), jnp.float32)
        for at in tiles:
            for cols in quarters:
                value = basis[group, j, at, cols]
                if not first:
                    value = value - alpha * basis[group, before, at, cols] - gamma * basis[group, earlier, at, cols]
                    basis[group, j, at, cols] = value
                norm_part = norm_part + folded(value * value)
        norm = total_of([norm_part])
        if first:
            for k in range(1, n):
                piece_copy(1, group, k).wait_recv()
            if group == 1:
                send_early(0)

        def back(at, cols):
            return dot3((mid_high[:, at], mid_low[:, at]), (from_high[at, cols], from_low[at, cols]))

        zero, two = back(quarters[0], slice(0, quarter)), back(quarters[1], slice(0, quarter))
        odds = back(odd, slice(0, 2 * quarter))
        alpha_part, square_part = jnp.zeros((SUBLANES, quarter), jnp.float32), jnp.zeros((SUBLANES, quarter), jnp.float32)
        for at in tiles:
            plus, minus, one, three = zero[at] + two[at], zero[at] - two[at], odds[at, :quarter], odds[at, quarter:]
            q = []
            for cols, value in zip(quarters, (plus + one, minus + three, plus - one, minus - three)):
                here = basis[group, j, at, cols]
                new = energy[group, at, cols] * here - value
                basis[group, j + 1, at, cols] = new
                alpha_part = alpha_part + folded(here * new)
                square_part = square_part + folded(new * new)
                q.append(new)
            if not final:
                spread_quarters(at, q)
        return alpha_part, square_part, norm, results[2], message

    nothing, no_part = jnp.zeros((1, 1), jnp.float32), jnp.zeros((SUBLANES, quarter), jnp.float32)
    results = (no_part, no_part, nothing, nothing, jnp.zeros((1, LANES), jnp.float32))
    steps = GROUPS * ITERS
    for group in range(GROUPS):
        results = step(group * ITERS, results, first=True)
        stop = (group + 1) * ITERS - (group == GROUPS - 1)
        results = lax.fori_loop(group * ITERS + 1, stop, step, results)
    results = step(steps - 1, results, final=True)
    send_message(1, settle(steps, results)[2])
    send_early(1)

    def tables_of(stage):
        for k in range(1, members):
            message_copy(stage, k).wait_recv()
        for r in range(members):
            gathered[stage, r:r + 1, :] = sums[stage, r]
        table = gathered[stage]
        norms = jnp.where(wide_lane < LANES // 2, table, 0.0)
        return norms, pltpu.roll(table, LANES // 2, 1), jnp.where(order > 0, norms * inverse_of(pltpu.roll(norms, 1, 1)), 0.0)

    wide_lane = lax.broadcasted_iota(jnp.int32, (members, LANES), 1)
    order = wide_lane % SUBLANES
    used = jnp.logical_and(order <= ITERS, wide_lane < SUBLANES * GROUPS)

    def image_of(tables, vector):
        diagonal, coupling = tables[1:]
        raised = jnp.where(order > 0, pltpu.roll(vector, 1, 1), 0.0)
        lowered = jnp.where(order < ITERS, pltpu.roll(coupling * vector, LANES - 1, 1), 0.0)
        return jnp.where(used, raised + jnp.where(order < ITERS, diagonal, 0.0) * vector + lowered, 0.0)

    alphas, betas = jnp.zeros((1, LANES), jnp.float32), jnp.zeros((1, LANES), jnp.float32)
    tables = tables_of(0)
    vector, previous = jnp.where(jnp.logical_and(used, order == 0), 1.0, 0.0), jnp.zeros((members, LANES), jnp.float32)
    size = nothing
    for j in range(ITERS):
        if j == ITERS - 1:
            tables = tables_of(1)
        image = image_of(tables, vector)
        size_before, size = size, total_of([tables[0] * vector * vector])
        alpha = total_of([tables[0] * vector * image]) / size
        rest = image - alpha * vector
        if j > 0:
            ratio = size / size_before
            betas = jnp.where(lane == j - 1, jnp.sqrt(ratio), betas)
            rest = rest - ratio * previous
        alphas = jnp.where(lane == j, alpha, alphas)
        vector, previous = rest, vector
    norms, diagonal, coupling = tables
    top = ITERS - 1
    weights = vector - jnp.where(order == top, diagonal * pltpu.roll(vector, LANES - 1, 1), 0.0)
    weights = weights - jnp.where(order == top - 1, pltpu.roll(coupling, LANES - 1, 1) * pltpu.roll(vector, LANES - 2, 1), 0.0)
    size_before, size = size, total_of([norms * vector * vector])
    unit = 1.0 / jnp.sqrt(size / total_count)
    coef[0:1, :] = alphas
    coef[1:2, :] = jnp.where(lane == ITERS - 1, jnp.sqrt(size / size_before), betas)
    gathered[2] = weights

    def scales_of(owner):
        row = gathered[2, pl.ds(owner, 1), :]
        return [
            [jnp.sum(jnp.where(lane == SUBLANES * group + i, row, 0.0), axis=1, keepdims=True) * unit for i in range(ITERS + 1)]
            for group in range(GROUPS)
        ]

    scales = scales_of(rank)

    def own_value(group, at, cols):
        return sum((scales[group][i] * basis[group, i, at, cols] for i in range(1, ITERS + 1)), scales[group][0] * basis[group, 0, at, cols])

    every, late = slice(0, cells), slice(early_stop, cells)
    out_copies = []
    for k in range(1, n + 1):
        peer = (me + k) % n
        here = pl.multiple_of(peer * piece, piece)
        target, place = (outgoing, peer) if k < n else (land, me)
        target[place, early:piece, :] = own_value(0, pl.ds(here + early, piece - early), every)
        target[place, piece:, :] = own_value(1, pl.ds(here, piece), every)
        if k == n:
            target[place, :early, :] = own_value(0, pl.ds(here, early), every)
            continue
        areas = [(pl.ds(early, GROUPS * piece - early), pl.ds(0, cells))]
        if early_stop < cells:
            target[place, :early, late] = own_value(0, pl.ds(here, early), late)
            areas.append((pl.ds(0, early), pl.ds(early_stop, cells - early_stop)))
        for i, (at, cols) in enumerate(areas):
            copy = pltpu.make_async_remote_copy(
                src_ref=outgoing.at[peer, at, cols], dst_ref=land.at[me, at, cols], send_sem=out_send.at[i, k], recv_sem=out_recv.at[i, k],
                device_id={"grid": peer}, device_id_type=MESH)
            copy.start()
            out_copies.append(copy)
    for k in range(1, n):
        for part in range(len(EARLY_EIGHTHS)):
            early_copy(part, k).wait()
        peer = (me + n - k) % n
        scale = scales_of(band * n + peer)[0]
        value = scale[0] * packed[0, 0, peer, :early, :early_stop]
        for i in range(1, ITERS + 1):
            value = value + scale[i] * early_land[peer, i - 1, :, :early_stop]
        land[peer, :early, :early_stop] = value
    for group in range(GROUPS):
        for kind in range(2):
            for k in range(1, n):
                piece_copy(kind, group, k).wait_send()
    for stage in range(2):
        for k in range(1, members):
            message_copy(stage, k).wait_send()
    for copy in out_copies:
        copy.wait()


def unpack_kernel(halves, planes, land, coef, out, alphas, betas):
    owners, cells = land.shape[0], land.shape[2]
    upper = lax.broadcasted_iota(jnp.int32, (SUBLANES, cells), 0) < PART
    for owner in range(owners):
        at = slice(owner % halves * SUBLANES, (owner % halves + 1) * SUBLANES)
        for pair in range(planes // 2):
            here = slice(pair * SUBLANES, (pair + 1) * SUBLANES)
            one, two = land[owner, here, :], land[owner, slice(here.start + planes * PART, here.stop + planes * PART), :]
            out[0, owner // halves, 0, at, 2 * pair * cells:(2 * pair + 1) * cells] = jnp.where(upper, one, pltpu.roll(two, PART, 0))
            out[0, owner // halves, 0, at, (2 * pair + 1) * cells:(2 * pair + 2) * cells] = jnp.where(upper, pltpu.roll(one, PART, 0), two)
    alphas[0] = coef[0:1, :ITERS]
    betas[0] = coef[1:2, :ITERS]


def field_body(start, energies, sites, potential):
    grid_size = potential.shape[0]
    cells = grid_size * grid_size
    n, band_n = lax.axis_size("grid"), lax.axis_size("band")
    halves = start.shape[3] // SUBLANES
    planes = grid_size // n
    rows, piece, half_cells = grid_size * PART, planes * PART, cells // 2
    index = np.arange(grid_size)
    angle = (index[:, None] * index[None, :] % grid_size) * (2.0 * math.pi / grid_size)
    cas = np.cos(angle) + np.sin(angle)
    ordered = cas[frequency_order(grid_size)]
    half_grid = grid_size // 2
    forward_y = jnp.asarray(np.repeat(ordered.T[:half_grid], grid_size, axis=1), jnp.float32)
    back_y = jnp.asarray(np.repeat(ordered[:, :half_grid], grid_size, axis=1), jnp.float32)
    all_z = jnp.asarray(np.tile(cas, (1, grid_size)), jnp.float32)
    x_wide = np.kron(cas, np.eye(PART)).astype(np.float32)
    x_high = x_wide.astype(jnp.bfloat16)
    x_low = (x_wide - x_high.astype(np.float32)).astype(jnp.bfloat16)
    x_wide = jnp.asarray(np.concatenate([x_high, x_low, x_high], axis=1))
    vmem = pl.BlockSpec(memory_space=pltpu.VMEM)
    hbm = pl.BlockSpec(memory_space=pltpu.MemorySpace.HBM)
    f32, bf16 = jnp.float32, jnp.bfloat16
    dma = pltpu.SemaphoreType.DMA
    members = n * band_n
    land_shape = (n, GROUPS * piece, cells)
    operands = (start, energies, sites[:, 0], potential, forward_y, back_y, all_z, x_wide)
    operands = (pltpu.with_memory_space_constraint(value, pltpu.MemorySpace.HBM) for value in operands)
    land, coef = pl.pallas_call(
        functools.partial(recursion_kernel, (n, band_n, grid_size, halves)),
        out_shape=(jax.ShapeDtypeStruct(land_shape, f32), jax.ShapeDtypeStruct((2, LANES), f32)),
        in_specs=[hbm] * 8,
        out_specs=(vmem, vmem),
        scratch_shapes=[
            pltpu.SMEM((3,), jnp.int32),
            pltpu.VMEM((half_grid, cells), f32), pltpu.VMEM((grid_size, half_cells), f32), pltpu.VMEM((grid_size, cells), f32),
            pltpu.VMEM((rows, 3 * rows), bf16), pltpu.VMEM(potential.shape, f32),
            pltpu.VMEM((grid_size, cells), f32), pltpu.VMEM((grid_size, cells), f32),
            pltpu.VMEM(start.shape, f32), pltpu.VMEM(energies.shape, f32),
            pltpu.VMEM((2, GROUPS, n, piece, cells), f32),
            pltpu.VMEM((GROUPS, ITERS + 1, rows, cells), f32), pltpu.VMEM((GROUPS, rows, cells), f32),
            pltpu.VMEM((rows, cells), f32),
            pltpu.VMEM((half_cells, cells), bf16), pltpu.VMEM((half_cells, cells), bf16),
            pltpu.VMEM((cells, half_cells), bf16), pltpu.VMEM((cells, half_cells), bf16),
            pltpu.VMEM((rows, cells), bf16), pltpu.VMEM((rows, cells), bf16),
            pltpu.VMEM((rows, cells), bf16), pltpu.VMEM((rows, cells), bf16),
            pltpu.VMEM((2, rows, cells), f32), pltpu.VMEM(land_shape, f32),
            pltpu.VMEM((n, ITERS, piece // 2, cells), f32),
            pltpu.VMEM((2, members, 1, LANES), f32), pltpu.VMEM((3, members, LANES), f32),
            dma((6,)), dma((2,)), dma((2, GROUPS, n)), dma((2, GROUPS, n)), dma((2, n)), dma((2, n)),
            dma((2, members)), dma((2, members)), pltpu.SemaphoreType.REGULAR, dma((len(EARLY_EIGHTHS), n)), dma((len(EARLY_EIGHTHS), n)),
        ],
        compiler_params=pltpu.CompilerParams(collective_id=0, has_side_effects=True, vmem_limit_bytes=36 * 1024 * 1024),
    )(*operands)
    scalar = jax.ShapeDtypeStruct((1, 1, ITERS), f32)
    out, alphas, betas = pl.pallas_call(
        functools.partial(unpack_kernel, halves, planes),
        out_shape=(jax.ShapeDtypeStruct(start.shape, f32), scalar, scalar),
        in_specs=[vmem, vmem],
        out_specs=(vmem, vmem, vmem),
        compiler_params=pltpu.CompilerParams(vmem_limit_bytes=8 * 1024 * 1024),
    )(land, coef)
    return alphas, betas, out


def body(start, energies, sites, potential):
    atoms, cores, pols, bands, _ = start.shape
    grid_size = potential.shape[0]
    n = lax.axis_size("grid")
    whole_fields = (
        atoms == 1 and pols == 1 and bands % SUBLANES == 0 and cores * bands == SUBLANES * n
        and grid_size % (2 * SUBLANES) == 0 and grid_size % (2 * n) == 0
        and grid_size * grid_size % (4 * LANES) == 0 and n * lax.axis_size("band") % SUBLANES == 0
    )
    return (field_body if whole_fields else plane_body)(start, energies, sites, potential)


def solution(mesh):
    in_specs = (P(None, None, None, "band", "grid"), P(None, "band", "grid"), P(), P())
    out_specs = (P(), P(), P(None, None, None, "band", "grid"))
    return jax.shard_map(body, mesh=mesh, in_specs=in_specs, out_specs=out_specs, check_vma=False)
```

```python
import functools
import math

import jax
import jax.numpy as jnp
import numpy as np
from jax import lax
from jax.experimental import pallas as pl
from jax.experimental.pallas import tpu as pltpu
from jax.sharding import PartitionSpec as P

ITERS = 4


precise_mode = lax.Precision.HIGHEST


def cas_table(grid_size):
    cells = jnp.arange(grid_size, dtype=jnp.int32)
    phase = cells[:, None] * cells[None, :] % grid_size
    angle = phase.astype(jnp.float32) * (2.0 * math.pi / grid_size)
    return jnp.cos(angle) + jnp.sin(angle)


def shift_axis(field_part, offset, axis_number):
    length = field_part.shape[axis_number]
    doubled = jnp.concatenate([field_part, field_part], axis=axis_number)
    first_index = (length - offset) % length
    return lax.dynamic_slice_in_dim(doubled, first_index, length, axis_number)


def expand_coef(values):
    return values[:, None, :, None, None]


def plane_body(start, energies, sites, potential):
    grid_size = potential.shape[0]
    volume = grid_size * grid_size * grid_size
    atom_count, core_count, pol_count, band_local, kpoint_local = start.shape
    plane_count = grid_size // lax.axis_size("grid")
    position = lax.axis_index("grid")
    chain_count = core_count * pol_count * band_local
    field_count = atom_count * chain_count
    total_count = (
        core_count * band_local * lax.axis_size("band") * kpoint_local * lax.axis_size("grid")
    )
    cas_grid = cas_table(grid_size)
    shifted = shift_axis(potential, sites[0, 0], 0)
    shifted = shift_axis(shifted, sites[1, 0], 1)
    shifted = shift_axis(shifted, sites[2, 0], 2)
    tables = [shifted]
    shifted_all = jnp.stack(tables, axis=-1)
    slab_table = lax.dynamic_slice_in_dim(shifted_all, position * plane_count, plane_count, 1)

    def moment(left, right):
        return jnp.sum(left * right, axis=(1, 3, 4)) / total_count

    start_sum = lax.psum(moment(start, start), ("grid", "band"))
    lanczos = start / expand_coef(jnp.sqrt(start_sum))
    previous = jnp.zeros_like(start)
    beta_prev = jnp.zeros((atom_count, pol_count), jnp.float32)
    alpha_list = []
    beta_list = []
    for iteration in range(ITERS):
        spread_fields = lanczos.reshape(atom_count, chain_count, plane_count, grid_size, grid_size)
        spread_over_z = jnp.einsum(
            "arpyz,wz->pywar", spread_fields, cas_grid, precision=precise_mode
        )
        spread_over_y = jnp.einsum(
            "pywar,uy->puwar", spread_over_z, cas_grid, precision=precise_mode
        )
        direct_spectrum = lax.all_to_all(
            spread_over_y.reshape(plane_count, grid_size, grid_size, field_count),
            "grid",
            split_axis=1,
            concat_axis=0,
            tiled=True,
        )
        field_shape = direct_spectrum.shape
        over_x = jnp.einsum("xvwf,tx->tvwf", direct_spectrum, cas_grid, precision=precise_mode)
        split_view = over_x.reshape(
            field_shape[0], field_shape[1], field_shape[2], atom_count, chain_count
        )
        scaled = split_view * slab_table[..., None]
        back_x = jnp.einsum("tvwar,xt->xvwar", scaled, cas_grid, precision=precise_mode)
        weighted = back_x.reshape(field_shape)
        direct_returned = lax.all_to_all(weighted, "grid", split_axis=0, concat_axis=1, tiled=True)
        fields = direct_returned.reshape(plane_count, grid_size, grid_size, atom_count, chain_count)
        over_z = jnp.einsum("pvwar,zw->pvzar", fields, cas_grid, precision=precise_mode)
        over_y = jnp.einsum("pvzar,yv->arpyz", over_z, cas_grid, precision=precise_mode)
        applied = energies[None, :, None] * lanczos - over_y.reshape(start.shape) / volume
        moments_all = lax.psum(
            (
                moment(lanczos, applied),
                moment(applied, applied),
                moment(lanczos, lanczos),
                moment(previous, previous),
                moment(previous, applied),
                moment(lanczos, previous),
            ),
            ("grid", "band"),
        )
        alpha_now = moments_all[0]
        square = (
            moments_all[1]
            + alpha_now * alpha_now * moments_all[2]
            + beta_prev * beta_prev * moments_all[3]
        )
        square = square - 2.0 * alpha_now * moments_all[0] - 2.0 * beta_prev * moments_all[4]
        square = square + 2.0 * alpha_now * beta_prev * moments_all[5]
        beta_now = jnp.sqrt(square)
        remainder = applied - expand_coef(alpha_now) * lanczos - expand_coef(beta_prev) * previous
        previous = lanczos
        lanczos = remainder / expand_coef(beta_now)
        beta_prev = beta_now
        alpha_list.append(alpha_now)
        beta_list.append(beta_now)
    return (jnp.stack(alpha_list, axis=2), jnp.stack(beta_list, axis=2), lanczos)


MESH = pl.DeviceIdType.MESH
LANES = 128
SUBLANES = 8
GROUPS = 2
EARLY_EIGHTHS = (4, 3)
PART = SUBLANES // GROUPS


def split(value):
    high = value.astype(jnp.bfloat16)
    return high, (value - high.astype(jnp.float32)).astype(jnp.bfloat16)


def dot3(left, right):
    left_high, left_low = left
    right_high, right_low = right
    left = jnp.concatenate([left_high, left_low, left_high], axis=1)
    right = jnp.concatenate([right_high, right_high, right_low], axis=0)
    return jnp.dot(left, right, preferred_element_type=jnp.float32)


def shifted_potential(table, sites, grid_size):
    cells = grid_size * grid_size
    lane = lax.broadcasted_iota(jnp.int32, table.shape, 1) % grid_size
    for axis in range(3):
        step = 1
        while step < grid_size:
            if axis == 0:
                moved = pltpu.roll(table, step, 0)
            elif axis == 1:
                moved = pltpu.roll(table, step * grid_size, 1)
            else:
                moved = jnp.where(
                    lane >= step,
                    pltpu.roll(table, step, 1),
                    pltpu.roll(table, cells - grid_size + step, 1),
                )
            flag = jnp.full(table.shape, sites[axis] // step % 2, jnp.int32)
            table = jnp.where(flag == 1, moved, table)
            step *= 2
    return table


def total_of(parts):
    total = parts[0]
    for part in parts[1:]:
        total = total + part
    return jnp.sum(jnp.sum(total, axis=0, keepdims=True), axis=1, keepdims=True)


def inverse_of(value):
    return jnp.where(value > 0.0, 1.0 / jnp.where(value > 0.0, value, 1.0), 0.0)


def frequency_order(grid_size):
    cells = np.arange(grid_size)
    return np.concatenate([cells[0::4], cells[2::4], cells[1::2]])


def recursion_kernel(
    sizes, start, energies, sites, pot, forward_y, back_y, all_z, x_far,
    land, coef,
    sites_here, forward_y_here, back_y_here, all_z_here, x_wide, pot_here, pot_flat, pot_order,
    start_here, energy_here, packed, basis, energy, site_table,
    to_high, to_low, from_high, from_low, vec_high, vec_low, mid_high, mid_low, past,
    outgoing, early_land, sums, gathered,
    table_sem, load_sem, send_sem, recv_sem, out_send, out_recv, sum_send, sum_recv, plane_sem, early_send, early_recv,
):
    n, band_n, grid_size, halves = sizes
    me = lax.axis_index("grid")
    band = lax.axis_index("band")
    rank = band * n + me
    members = n * band_n
    cells = grid_size * grid_size
    planes = grid_size // n
    rows = grid_size * PART
    piece = planes * PART
    early = piece // 2
    quarter = cells // 4
    total_count = float(grid_size * SUBLANES * cells * members)

    load_copies = [
        pltpu.make_async_copy(source, target, load_sem.at[i])
        for i, (source, target) in enumerate(((start, start_here), (energies, energy_here)))
    ]
    table_copies = [
        pltpu.make_async_copy(source, target, table_sem.at[i])
        for i, (source, target) in enumerate((
            (forward_y, forward_y_here), (back_y, back_y_here), (all_z, all_z_here), (x_far, x_wide), (pot, pot_here), (sites, sites_here)))
    ]
    load_copies[0].start()
    barrier = pltpu.get_barrier_semaphore()
    for k in range(1, band_n):
        pl.semaphore_signal(barrier, inc=1, device_id={"band": (band + k) % band_n}, device_id_type=MESH)
    for k in range(1, n):
        pl.semaphore_signal(barrier, inc=1, device_id={"grid": (me + k) % n}, device_id_type=MESH)

    upper = lax.broadcasted_iota(jnp.int32, (SUBLANES, cells), 0) < PART

    def pack(kind):
        def pack_owner(owner, carry):
            at = pl.ds(pl.multiple_of(owner % halves * SUBLANES, SUBLANES), SUBLANES)
            for pair in range(planes // 2):
                first, second = slice(2 * pair * cells, (2 * pair + 1) * cells), slice((2 * pair + 1) * cells, (2 * pair + 2) * cells)
                if kind == 0:
                    one, two = start_here[0, owner // halves, 0, at, first], start_here[0, owner // halves, 0, at, second]
                else:
                    one, two = energy_here[owner // halves, at, first], energy_here[owner // halves, at, second]
                here = slice(pair * SUBLANES, (pair + 1) * SUBLANES)
                packed[kind, 0, owner, here, :] = jnp.where(upper, one, pltpu.roll(two, PART, 0))
                packed[kind, 1, owner, here, :] = jnp.where(upper, pltpu.roll(one, PART, 0), two)
            return carry

        lax.fori_loop(0, n, pack_owner, 0)

    my_rows = pl.ds(pl.multiple_of(me * piece, piece), piece)

    def piece_copy(kind, group, k):
        peer = (me + k) % n
        target = basis.at[group, 0, my_rows, :] if kind == 0 else energy.at[group, my_rows, :]
        return pltpu.make_async_remote_copy(
            src_ref=packed.at[kind, group, peer], dst_ref=target, send_sem=send_sem.at[kind, group, k],
            recv_sem=recv_sem.at[kind, group, k], device_id={"grid": peer}, device_id_type=MESH)

    load_copies[0].wait()
    for copy in load_copies[1:] + table_copies:
        copy.start()
    pack(0)
    pl.semaphore_wait(barrier, n + band_n - 2)
    for k in range(1, n):
        piece_copy(0, 0, k).start()
    load_copies[1].wait()
    pack(1)
    for kind, group in ((1, 0), (0, 1), (1, 1)):
        for k in range(1, n):
            piece_copy(kind, group, k).start()
    for k in range(1, band_n):
        pl.semaphore_signal(plane_sem, inc=1, device_id={"band": (band + k) % band_n}, device_id_type=MESH)
    for group in range(GROUPS):
        basis[group, 0, my_rows, :] = packed[0, group, me]
        energy[group, my_rows, :] = packed[1, group, me]

    for copy in table_copies:
        copy.wait()

    def forward_rows(y, carry):
        high, low = split(forward_y_here[pl.ds(y, 1), :] * all_z_here[...])
        at = pl.ds(pl.multiple_of(y * grid_size, grid_size), grid_size)
        to_high[at, :] = high
        to_low[at, :] = low
        return carry

    def back_rows(v, carry):
        high, low = split(back_y_here[pl.ds(v, 1), :] * all_z_here[:, : 2 * quarter])
        at = pl.ds(pl.multiple_of(v * grid_size, grid_size), grid_size)
        from_high[at, :] = high
        from_low[at, :] = low
        return carry

    lax.fori_loop(0, grid_size // 2, forward_rows, 0)
    lax.fori_loop(0, grid_size, back_rows, 0)
    for y in range(grid_size):
        pot_flat[:, y * grid_size:(y + 1) * grid_size] = pot_here[:, y, :]
    pot_flat[...] = shifted_potential(pot_flat[...], sites_here, grid_size) * (1.0 / (grid_size * cells))
    for place, v in enumerate(frequency_order(grid_size)):
        pot_order[:, place * grid_size:(place + 1) * grid_size] = pot_flat[:, int(v) * grid_size:(int(v) + 1) * grid_size]
    for x in range(grid_size):
        site_table[PART * x:PART * (x + 1), :] = jnp.broadcast_to(pot_order[x:x + 1, :], (PART, cells))

    pl.semaphore_wait(plane_sem, band_n - 1)

    quarters = [slice(i * quarter, (i + 1) * quarter) for i in range(4)]
    odd = slice(2 * quarter, 4 * quarter)
    lane = lax.broadcasted_iota(jnp.int32, (1, LANES), 1)
    tall = 2 * SUBLANES

    def lane_is(place):
        return lane == jnp.full((1, LANES), place, jnp.int32)

    def folded(product):
        return sum((product[i:i + SUBLANES] for i in range(SUBLANES, product.shape[0], SUBLANES)), product[:SUBLANES])

    def times_x(value):
        high, low = split(value)
        return jnp.dot(x_wide[...], jnp.concatenate([high, high, low], axis=0), preferred_element_type=jnp.float32)

    eighth = cells // 8
    early_columns = [pl.ds(sum(EARLY_EIGHTHS[:i]) * eighth, EARLY_EIGHTHS[i] * eighth) for i in range(len(EARLY_EIGHTHS))]
    early_stop = sum(EARLY_EIGHTHS) * eighth

    def early_copy(part, k):
        peer = (me + k) % n
        at = pl.ds(pl.multiple_of(peer * piece, SUBLANES), early)
        return pltpu.make_async_remote_copy(
            src_ref=basis.at[0, pl.ds(1, ITERS), at, early_columns[part]], dst_ref=early_land.at[me, :, :, early_columns[part]],
            send_sem=early_send.at[part, k], recv_sem=early_recv.at[part, k], device_id={"grid": peer}, device_id_type=MESH)

    def send_early(part):
        for k in range(1, n):
            early_copy(part, k).start()

    def message_copy(stage, k):
        return pltpu.make_async_remote_copy(
            src_ref=sums.at[stage, rank], dst_ref=sums.at[stage, rank], send_sem=sum_send.at[stage, k], recv_sem=sum_recv.at[stage, k],
            device_id={"grid": (me + k % n) % n, "band": (band + k // n) % band_n}, device_id_type=MESH)

    far_first = sorted(range(1, members), key=lambda k: -min(k // n, band_n - k // n))

    def send_message(stage, message):
        sums[stage, rank] = message
        for k in far_first:
            message_copy(stage, k).start()

    tiles = [slice(r, r + tall) for r in range(0, rows, tall)]

    def spread_quarters(at, q):
        even, other = q[0] + q[2], q[1] + q[3]
        for cols, value in zip(quarters, (even + other, even - other, q[0] - q[2], q[1] - q[3])):
            vec_high[at, cols], vec_low[at, cols] = split(value)

    def settle(t, results):
        alpha_part, square_part, norm, norm_before, message = results
        j = (t + ITERS - 1) % ITERS
        alpha = total_of([alpha_part]) * inverse_of(norm)
        gamma = jnp.where(jnp.full((1, 1), j, jnp.int32) == 0, 0.0, norm * inverse_of(norm_before))
        norm_after = jnp.maximum(total_of([square_part]) - alpha * alpha * norm - gamma * norm, 0.0)
        place = SUBLANES * ((t + ITERS - 1) // ITERS - 1) + j
        message = jnp.where(lane_is(place), norm, message)
        message = jnp.where(lane_is(place + 1), norm_after, message)
        message = jnp.where(lane_is(place + LANES // 2), alpha, message)
        return alpha, gamma, message

    def step(t, results, first=False, final=False):
        alpha, gamma, message = settle(t, results)
        group, j = t // ITERS, t % ITERS
        if final:
            send_message(0, message)
        if first:
            for k in range(1, n):
                piece_copy(0, group, k).wait_recv()
            for at in tiles:
                spread_quarters(at, [basis[group, 0, at, cols] for cols in quarters])
        else:
            before, earlier, now = j - 1, jnp.maximum(j - 2, 0), j % 2

        def forward(i):
            cols = quarters[i]
            source, depth = (cols, quarter) if i < 2 else (odd, 2 * quarter)
            spectrum = dot3((vec_high[:, source], vec_low[:, source]), (to_high[:depth, cols], to_low[:depth, cols]))
            if first:
                past[0, :, cols] = spectrum
                past[1, :, cols] = jnp.zeros_like(spectrum)
            else:
                spectrum = spectrum - alpha * past[1 - now, :, cols] - gamma * past[now, :, cols]
                past[now, :, cols] = spectrum
            return spectrum

        def weigh(i, spectrum):
            return times_x(past[0 if first else now, :, quarters[i]]) * site_table[:, quarters[i]]

        def finish(i, spectrum):
            mid_high[:, quarters[i]], mid_low[:, quarters[i]] = split(times_x(spectrum))

        work = [forward(i) for i in range(4)]
        work = [weigh(i, work[i]) for i in range(4)]
        for i in range(4):
            finish(i, work[i])
        norm_part = jnp.zeros((SUBLANES, quarter), jnp.float32)
        for at in tiles:
            for cols in quarters:
                value = basis[group, j, at, cols]
                if not first:
                    value = value - alpha * basis[group, before, at, cols] - gamma * basis[group, earlier, at, cols]
                    basis[group, j, at, cols] = value
                norm_part = norm_part + folded(value * value)
        norm = total_of([norm_part])
        if first:
            for k in range(1, n):
                piece_copy(1, group, k).wait_recv()
            if group == 1:
                send_early(0)

        def back(at, cols):
            return dot3((mid_high[:, at], mid_low[:, at]), (from_high[at, cols], from_low[at, cols]))

        zero, two = back(quarters[0], slice(0, quarter)), back(quarters[1], slice(0, quarter))
        odds = back(odd, slice(0, 2 * quarter))
        alpha_part, square_part = jnp.zeros((SUBLANES, quarter), jnp.float32), jnp.zeros((SUBLANES, quarter), jnp.float32)
        for at in tiles:
            plus, minus, one, three = zero[at] + two[at], zero[at] - two[at], odds[at, :quarter], odds[at, quarter:]
            q = []
            for cols, value in zip(quarters, (plus + one, minus + three, plus - one, minus - three)):
                here = basis[group, j, at, cols]
                new = energy[group, at, cols] * here - value
                basis[group, j + 1, at, cols] = new
                alpha_part = alpha_part + folded(here * new)
                square_part = square_part + folded(new * new)
                q.append(new)
            if not final:
                spread_quarters(at, q)
        return alpha_part, square_part, norm, results[2], message

    nothing, no_part = jnp.zeros((1, 1), jnp.float32), jnp.zeros((SUBLANES, quarter), jnp.float32)
    results = (no_part, no_part, nothing, nothing, jnp.zeros((1, LANES), jnp.float32))
    steps = GROUPS * ITERS
    for group in range(GROUPS):
        results = step(group * ITERS, results, first=True)
        stop = (group + 1) * ITERS - (group == GROUPS - 1)
        results = lax.fori_loop(group * ITERS + 1, stop, step, results)
    results = step(steps - 1, results, final=True)
    send_message(1, settle(steps, results)[2])
    send_early(1)

    def tables_of(stage):
        for k in range(1, members):
            message_copy(stage, k).wait_recv()
        for r in range(members):
            gathered[stage, r:r + 1, :] = sums[stage, r]
        table = gathered[stage]
        norms = jnp.where(wide_lane < LANES // 2, table, 0.0)
        return norms, pltpu.roll(table, LANES // 2, 1), jnp.where(order > 0, norms * inverse_of(pltpu.roll(norms, 1, 1)), 0.0)

    wide_lane = lax.broadcasted_iota(jnp.int32, (members, LANES), 1)
    order = wide_lane % SUBLANES
    used = jnp.logical_and(order <= ITERS, wide_lane < SUBLANES * GROUPS)

    def image_of(tables, vector):
        diagonal, coupling = tables[1:]
        raised = jnp.where(order > 0, pltpu.roll(vector, 1, 1), 0.0)
        lowered = jnp.where(order < ITERS, pltpu.roll(coupling * vector, LANES - 1, 1), 0.0)
        return jnp.where(used, raised + jnp.where(order < ITERS, diagonal, 0.0) * vector + lowered, 0.0)

    alphas, betas = jnp.zeros((1, LANES), jnp.float32), jnp.zeros((1, LANES), jnp.float32)
    tables = tables_of(0)
    vector, previous = jnp.where(jnp.logical_and(used, order == 0), 1.0, 0.0), jnp.zeros((members, LANES), jnp.float32)
    size = nothing
    for j in range(ITERS):
        if j == ITERS - 1:
            tables = tables_of(1)
        image = image_of(tables, vector)
        size_before, size = size, total_of([tables[0] * vector * vector])
        alpha = total_of([tables[0] * vector * image]) / size
        rest = image - alpha * vector
        if j > 0:
            ratio = size / size_before
            betas = jnp.where(lane == j - 1, jnp.sqrt(ratio), betas)
            rest = rest - ratio * previous
        alphas = jnp.where(lane == j, alpha, alphas)
        vector, previous = rest, vector
    norms, diagonal, coupling = tables
    top = ITERS - 1
    weights = vector - jnp.where(order == top, diagonal * pltpu.roll(vector, LANES - 1, 1), 0.0)
    weights = weights - jnp.where(order == top - 1, pltpu.roll(coupling, LANES - 1, 1) * pltpu.roll(vector, LANES - 2, 1), 0.0)
    size_before, size = size, total_of([norms * vector * vector])
    unit = 1.0 / jnp.sqrt(size / total_count)
    coef[0:1, :] = alphas
    coef[1:2, :] = jnp.where(lane == ITERS - 1, jnp.sqrt(size / size_before), betas)
    gathered[2] = weights

    def scales_of(owner):
        row = gathered[2, pl.ds(owner, 1), :]
        return [
            [jnp.sum(jnp.where(lane == SUBLANES * group + i, row, 0.0), axis=1, keepdims=True) * unit for i in range(ITERS + 1)]
            for group in range(GROUPS)
        ]

    scales = scales_of(rank)

    def own_value(group, at, cols):
        return sum((scales[group][i] * basis[group, i, at, cols] for i in range(1, ITERS + 1)), scales[group][0] * basis[group, 0, at, cols])

    every, late = slice(0, cells), slice(early_stop, cells)
    out_copies = []
    for k in range(1, n + 1):
        peer = (me + k) % n
        here = pl.multiple_of(peer * piece, piece)
        target, place = (outgoing, peer) if k < n else (land, me)
        target[place, early:piece, :] = own_value(0, pl.ds(here + early, piece - early), every)
        target[place, piece:, :] = own_value(1, pl.ds(here, piece), every)
        if k == n:
            target[place, :early, :] = own_value(0, pl.ds(here, early), every)
            continue
        areas = [(pl.ds(early, GROUPS * piece - early), pl.ds(0, cells))]
        if early_stop < cells:
            target[place, :early, late] = own_value(0, pl.ds(here, early), late)
            areas.append((pl.ds(0, early), pl.ds(early_stop, cells - early_stop)))
        for i, (at, cols) in enumerate(areas):
            copy = pltpu.make_async_remote_copy(
                src_ref=outgoing.at[peer, at, cols], dst_ref=land.at[me, at, cols], send_sem=out_send.at[i, k], recv_sem=out_recv.at[i, k],
                device_id={"grid": peer}, device_id_type=MESH)
            copy.start()
            out_copies.append(copy)
    for k in range(1, n):
        for part in range(len(EARLY_EIGHTHS)):
            early_copy(part, k).wait()
        peer = (me + n - k) % n
        scale = scales_of(band * n + peer)[0]
        value = scale[0] * packed[0, 0, peer, :early, :early_stop]
        for i in range(1, ITERS + 1):
            value = value + scale[i] * early_land[peer, i - 1, :, :early_stop]
        land[peer, :early, :early_stop] = value
    for group in range(GROUPS):
        for kind in range(2):
            for k in range(1, n):
                piece_copy(kind, group, k).wait_send()
    for stage in range(2):
        for k in range(1, members):
            message_copy(stage, k).wait_send()
    for copy in out_copies:
        copy.wait()


def unpack_kernel(halves, planes, land, coef, out, alphas, betas):
    owners, cells = land.shape[0], land.shape[2]
    upper = lax.broadcasted_iota(jnp.int32, (SUBLANES, cells), 0) < PART
    for owner in range(owners):
        at = slice(owner % halves * SUBLANES, (owner % halves + 1) * SUBLANES)
        for pair in range(planes // 2):
            here = slice(pair * SUBLANES, (pair + 1) * SUBLANES)
            one, two = land[owner, here, :], land[owner, slice(here.start + planes * PART, here.stop + planes * PART), :]
            out[0, owner // halves, 0, at, 2 * pair * cells:(2 * pair + 1) * cells] = jnp.where(upper, one, pltpu.roll(two, PART, 0))
            out[0, owner // halves, 0, at, (2 * pair + 1) * cells:(2 * pair + 2) * cells] = jnp.where(upper, pltpu.roll(one, PART, 0), two)
    alphas[0] = coef[0:1, :ITERS]
    betas[0] = coef[1:2, :ITERS]


def field_body(start, energies, sites, potential):
    grid_size = potential.shape[0]
    cells = grid_size * grid_size
    n, band_n = lax.axis_size("grid"), lax.axis_size("band")
    halves = start.shape[3] // SUBLANES
    planes = grid_size // n
    rows, piece, half_cells = grid_size * PART, planes * PART, cells // 2
    index = np.arange(grid_size)
    angle = (index[:, None] * index[None, :] % grid_size) * (2.0 * math.pi / grid_size)
    cas = np.cos(angle) + np.sin(angle)
    ordered = cas[frequency_order(grid_size)]
    half_grid = grid_size // 2
    forward_y = jnp.asarray(np.repeat(ordered.T[:half_grid], grid_size, axis=1), jnp.float32)
    back_y = jnp.asarray(np.repeat(ordered[:, :half_grid], grid_size, axis=1), jnp.float32)
    all_z = jnp.asarray(np.tile(cas, (1, grid_size)), jnp.float32)
    x_wide = np.kron(cas, np.eye(PART)).astype(np.float32)
    x_high = x_wide.astype(jnp.bfloat16)
    x_low = (x_wide - x_high.astype(np.float32)).astype(jnp.bfloat16)
    x_wide = jnp.asarray(np.concatenate([x_high, x_low, x_high], axis=1))
    vmem = pl.BlockSpec(memory_space=pltpu.VMEM)
    hbm = pl.BlockSpec(memory_space=pltpu.MemorySpace.HBM)
    f32, bf16 = jnp.float32, jnp.bfloat16
    dma = pltpu.SemaphoreType.DMA
    members = n * band_n
    land_shape = (n, GROUPS * piece, cells)
    operands = (start, energies, sites[:, 0], potential, forward_y, back_y, all_z, x_wide)
    operands = (pltpu.with_memory_space_constraint(value, pltpu.MemorySpace.HBM) for value in operands)
    land, coef = pl.pallas_call(
        functools.partial(recursion_kernel, (n, band_n, grid_size, halves)),
        out_shape=(jax.ShapeDtypeStruct(land_shape, f32), jax.ShapeDtypeStruct((2, LANES), f32)),
        in_specs=[hbm] * 8,
        out_specs=(vmem, vmem),
        scratch_shapes=[
            pltpu.SMEM((3,), jnp.int32),
            pltpu.VMEM((half_grid, cells), f32), pltpu.VMEM((grid_size, half_cells), f32), pltpu.VMEM((grid_size, cells), f32),
            pltpu.VMEM((rows, 3 * rows), bf16), pltpu.VMEM(potential.shape, f32),
            pltpu.VMEM((grid_size, cells), f32), pltpu.VMEM((grid_size, cells), f32),
            pltpu.VMEM(start.shape, f32), pltpu.VMEM(energies.shape, f32),
            pltpu.VMEM((2, GROUPS, n, piece, cells), f32),
            pltpu.VMEM((GROUPS, ITERS + 1, rows, cells), f32), pltpu.VMEM((GROUPS, rows, cells), f32),
            pltpu.VMEM((rows, cells), f32),
            pltpu.VMEM((half_cells, cells), bf16), pltpu.VMEM((half_cells, cells), bf16),
            pltpu.VMEM((cells, half_cells), bf16), pltpu.VMEM((cells, half_cells), bf16),
            pltpu.VMEM((rows, cells), bf16), pltpu.VMEM((rows, cells), bf16),
            pltpu.VMEM((rows, cells), bf16), pltpu.VMEM((rows, cells), bf16),
            pltpu.VMEM((2, rows, cells), f32), pltpu.VMEM(land_shape, f32),
            pltpu.VMEM((n, ITERS, piece // 2, cells), f32),
            pltpu.VMEM((2, members, 1, LANES), f32), pltpu.VMEM((3, members, LANES), f32),
            dma((6,)), dma((2,)), dma((2, GROUPS, n)), dma((2, GROUPS, n)), dma((2, n)), dma((2, n)),
            dma((2, members)), dma((2, members)), pltpu.SemaphoreType.REGULAR, dma((len(EARLY_EIGHTHS), n)), dma((len(EARLY_EIGHTHS), n)),
        ],
        compiler_params=pltpu.CompilerParams(collective_id=0, has_side_effects=True, vmem_limit_bytes=36 * 1024 * 1024),
    )(*operands)
    scalar = jax.ShapeDtypeStruct((1, 1, ITERS), f32)
    out, alphas, betas = pl.pallas_call(
        functools.partial(unpack_kernel, halves, planes),
        out_shape=(jax.ShapeDtypeStruct(start.shape, f32), scalar, scalar),
        in_specs=[vmem, vmem],
        out_specs=(vmem, vmem, vmem),
        compiler_params=pltpu.CompilerParams(vmem_limit_bytes=8 * 1024 * 1024),
    )(land, coef)
    return alphas, betas, out


def body(start, energies, sites, potential):
    atoms, cores, pols, bands, _ = start.shape
    grid_size = potential.shape[0]
    n = lax.axis_size("grid")
    whole_fields = (
        atoms == 1 and pols == 1 and bands % SUBLANES == 0 and cores * bands == SUBLANES * n
        and grid_size % (2 * SUBLANES) == 0 and grid_size % (2 * n) == 0
        and grid_size * grid_size % (4 * LANES) == 0 and n * lax.axis_size("band") % SUBLANES == 0
    )
    return (field_body if whole_fields else plane_body)(start, energies, sites, potential)


def solution(mesh):
    in_specs = (P(None, None, None, "band", "grid"), P(None, "band", "grid"), P(), P())
    out_specs = (P(), P(), P(None, None, None, "band", "grid"))
    return jax.shard_map(body, mesh=mesh, in_specs=in_specs, out_specs=out_specs, check_vma=False)
```

```python
import functools
import math

import jax
import jax.numpy as jnp
import numpy as np
from jax import lax
from jax.experimental import pallas as pl
from jax.experimental.pallas import tpu as pltpu
from jax.sharding import PartitionSpec as P

ITERS = 4


precise_mode = lax.Precision.HIGHEST


def cas_table(grid_size):
    cells = jnp.arange(grid_size, dtype=jnp.int32)
    phase = cells[:, None] * cells[None, :] % grid_size
    angle = phase.astype(jnp.float32) * (2.0 * math.pi / grid_size)
    return jnp.cos(angle) + jnp.sin(angle)


def shift_axis(field_part, offset, axis_number):
    length = field_part.shape[axis_number]
    doubled = jnp.concatenate([field_part, field_part], axis=axis_number)
    first_index = (length - offset) % length
    return lax.dynamic_slice_in_dim(doubled, first_index, length, axis_number)


def expand_coef(values):
    return values[:, None, :, None, None]


def plane_body(start, energies, sites, potential):
    grid_size = potential.shape[0]
    volume = grid_size * grid_size * grid_size
    atom_count, core_count, pol_count, band_local, kpoint_local = start.shape
    plane_count = grid_size // lax.axis_size("grid")
    position = lax.axis_index("grid")
    chain_count = core_count * pol_count * band_local
    field_count = atom_count * chain_count
    total_count = (
        core_count * band_local * lax.axis_size("band") * kpoint_local * lax.axis_size("grid")
    )
    cas_grid = cas_table(grid_size)
    shifted = shift_axis(potential, sites[0, 0], 0)
    shifted = shift_axis(shifted, sites[1, 0], 1)
    shifted = shift_axis(shifted, sites[2, 0], 2)
    tables = [shifted]
    shifted_all = jnp.stack(tables, axis=-1)
    slab_table = lax.dynamic_slice_in_dim(shifted_all, position * plane_count, plane_count, 1)

    def moment(left, right):
        return jnp.sum(left * right, axis=(1, 3, 4)) / total_count

    start_sum = lax.psum(moment(start, start), ("grid", "band"))
    lanczos = start / expand_coef(jnp.sqrt(start_sum))
    previous = jnp.zeros_like(start)
    beta_prev = jnp.zeros((atom_count, pol_count), jnp.float32)
    alpha_list = []
    beta_list = []
    for iteration in range(ITERS):
        spread_fields = lanczos.reshape(atom_count, chain_count, plane_count, grid_size, grid_size)
        spread_over_z = jnp.einsum(
            "arpyz,wz->pywar", spread_fields, cas_grid, precision=precise_mode
        )
        spread_over_y = jnp.einsum(
            "pywar,uy->puwar", spread_over_z, cas_grid, precision=precise_mode
        )
        direct_spectrum = lax.all_to_all(
            spread_over_y.reshape(plane_count, grid_size, grid_size, field_count),
            "grid",
            split_axis=1,
            concat_axis=0,
            tiled=True,
        )
        field_shape = direct_spectrum.shape
        over_x = jnp.einsum("xvwf,tx->tvwf", direct_spectrum, cas_grid, precision=precise_mode)
        split_view = over_x.reshape(
            field_shape[0], field_shape[1], field_shape[2], atom_count, chain_count
        )
        scaled = split_view * slab_table[..., None]
        back_x = jnp.einsum("tvwar,xt->xvwar", scaled, cas_grid, precision=precise_mode)
        weighted = back_x.reshape(field_shape)
        direct_returned = lax.all_to_all(weighted, "grid", split_axis=0, concat_axis=1, tiled=True)
        fields = direct_returned.reshape(plane_count, grid_size, grid_size, atom_count, chain_count)
        over_z = jnp.einsum("pvwar,zw->pvzar", fields, cas_grid, precision=precise_mode)
        over_y = jnp.einsum("pvzar,yv->arpyz", over_z, cas_grid, precision=precise_mode)
        applied = energies[None, :, None] * lanczos - over_y.reshape(start.shape) / volume
        moments_all = lax.psum(
            (
                moment(lanczos, applied),
                moment(applied, applied),
                moment(lanczos, lanczos),
                moment(previous, previous),
                moment(previous, applied),
                moment(lanczos, previous),
            ),
            ("grid", "band"),
        )
        alpha_now = moments_all[0]
        square = (
            moments_all[1]
            + alpha_now * alpha_now * moments_all[2]
            + beta_prev * beta_prev * moments_all[3]
        )
        square = square - 2.0 * alpha_now * moments_all[0] - 2.0 * beta_prev * moments_all[4]
        square = square + 2.0 * alpha_now * beta_prev * moments_all[5]
        beta_now = jnp.sqrt(square)
        remainder = applied - expand_coef(alpha_now) * lanczos - expand_coef(beta_prev) * previous
        previous = lanczos
        lanczos = remainder / expand_coef(beta_now)
        beta_prev = beta_now
        alpha_list.append(alpha_now)
        beta_list.append(beta_now)
    return (jnp.stack(alpha_list, axis=2), jnp.stack(beta_list, axis=2), lanczos)


MESH = pl.DeviceIdType.MESH
LANES = 128
SUBLANES = 8
GROUPS = 2
EARLY_EIGHTHS = (4, 3)
PART = SUBLANES // GROUPS


def split(value):
    high = value.astype(jnp.bfloat16)
    return high, (value - high.astype(jnp.float32)).astype(jnp.bfloat16)


def dot3(left, right):
    left_high, left_low = left
    right_high, right_low = right
    left = jnp.concatenate([left_high, left_low, left_high], axis=1)
    right = jnp.concatenate([right_high, right_high, right_low], axis=0)
    return jnp.dot(left, right, preferred_element_type=jnp.float32)


def shifted_potential(table, sites, grid_size):
    cells = grid_size * grid_size
    lane = lax.broadcasted_iota(jnp.int32, table.shape, 1) % grid_size
    for axis in range(3):
        step = 1
        while step < grid_size:
            if axis == 0:
                moved = pltpu.roll(table, step, 0)
            elif axis == 1:
                moved = pltpu.roll(table, step * grid_size, 1)
            else:
                moved = jnp.where(
                    lane >= step,
                    pltpu.roll(table, step, 1),
                    pltpu.roll(table, cells - grid_size + step, 1),
                )
            flag = jnp.full(table.shape, sites[axis] // step % 2, jnp.int32)
            table = jnp.where(flag == 1, moved, table)
            step *= 2
    return table


def total_of(parts):
    total = parts[0]
    for part in parts[1:]:
        total = total + part
    return jnp.sum(jnp.sum(total, axis=0, keepdims=True), axis=1, keepdims=True)


def inverse_of(value):
    return jnp.where(value > 0.0, 1.0 / jnp.where(value > 0.0, value, 1.0), 0.0)


def frequency_order(grid_size):
    cells = np.arange(grid_size)
    return np.concatenate([cells[0::4], cells[2::4], cells[1::2]])


def recursion_kernel(
    sizes, start, energies, sites, pot, forward_y, back_y, all_z, x_far,
    land, coef,
    sites_here, forward_y_here, back_y_here, all_z_here, x_wide, pot_here, pot_flat, pot_order,
    start_here, energy_here, packed, basis, energy, site_table,
    to_high, to_low, from_high, from_low, vec_high, vec_low, mid_high, mid_low, past,
    outgoing, early_land, sums, gathered,
    table_sem, load_sem, send_sem, recv_sem, out_send, out_recv, sum_send, sum_recv, plane_sem, early_send, early_recv,
):
    n, band_n, grid_size, halves = sizes
    me = lax.axis_index("grid")
    band = lax.axis_index("band")
    rank = band * n + me
    members = n * band_n
    cells = grid_size * grid_size
    planes = grid_size // n
    rows = grid_size * PART
    piece = planes * PART
    early = piece // 2
    quarter = cells // 4
    total_count = float(grid_size * SUBLANES * cells * members)

    load_copies = [
        pltpu.make_async_copy(source, target, load_sem.at[i])
        for i, (source, target) in enumerate(((start, start_here), (energies, energy_here)))
    ]
    table_copies = [
        pltpu.make_async_copy(source, target, table_sem.at[i])
        for i, (source, target) in enumerate((
            (forward_y, forward_y_here), (back_y, back_y_here), (all_z, all_z_here), (x_far, x_wide), (pot, pot_here), (sites, sites_here)))
    ]
    load_copies[0].start()
    barrier = pltpu.get_barrier_semaphore()
    for k in range(1, band_n):
        pl.semaphore_signal(barrier, inc=1, device_id={"band": (band + k) % band_n}, device_id_type=MESH)
    for k in range(1, n):
        pl.semaphore_signal(barrier, inc=1, device_id={"grid": (me + k) % n}, device_id_type=MESH)

    upper = lax.broadcasted_iota(jnp.int32, (SUBLANES, cells), 0) < PART

    def pack(kind):
        def pack_owner(owner, carry):
            at = pl.ds(pl.multiple_of(owner % halves * SUBLANES, SUBLANES), SUBLANES)
            for pair in range(planes // 2):
                first, second = slice(2 * pair * cells, (2 * pair + 1) * cells), slice((2 * pair + 1) * cells, (2 * pair + 2) * cells)
                if kind == 0:
                    one, two = start_here[0, owner // halves, 0, at, first], start_here[0, owner // halves, 0, at, second]
                else:
                    one, two = energy_here[owner // halves, at, first], energy_here[owner // halves, at, second]
                here = slice(pair * SUBLANES, (pair + 1) * SUBLANES)
                packed[kind, 0, owner, here, :] = jnp.where(upper, one, pltpu.roll(two, PART, 0))
                packed[kind, 1, owner, here, :] = jnp.where(upper, pltpu.roll(one, PART, 0), two)
            return carry

        lax.fori_loop(0, n, pack_owner, 0)

    my_rows = pl.ds(pl.multiple_of(me * piece, piece), piece)

    def piece_copy(kind, group, k):
        peer = (me + k) % n
        target = basis.at[group, 0, my_rows, :] if kind == 0 else energy.at[group, my_rows, :]
        return pltpu.make_async_remote_copy(
            src_ref=packed.at[kind, group, peer], dst_ref=target, send_sem=send_sem.at[kind, group, k],
            recv_sem=recv_sem.at[kind, group, k], device_id={"grid": peer}, device_id_type=MESH)

    load_copies[0].wait()
    for copy in load_copies[1:] + table_copies:
        copy.start()
    pack(0)
    pl.semaphore_wait(barrier, n + band_n - 2)
    for k in range(1, n):
        piece_copy(0, 0, k).start()
    load_copies[1].wait()
    pack(1)
    for kind, group in ((1, 0), (0, 1), (1, 1)):
        for k in range(1, n):
            piece_copy(kind, group, k).start()
    for k in range(1, band_n):
        pl.semaphore_signal(plane_sem, inc=1, device_id={"band": (band + k) % band_n}, device_id_type=MESH)
    for group in range(GROUPS):
        basis[group, 0, my_rows, :] = packed[0, group, me]
        energy[group, my_rows, :] = packed[1, group, me]

    for copy in table_copies:
        copy.wait()

    def forward_rows(y, carry):
        high, low = split(forward_y_here[pl.ds(y, 1), :] * all_z_here[...])
        at = pl.ds(pl.multiple_of(y * grid_size, grid_size), grid_size)
        to_high[at, :] = high
        to_low[at, :] = low
        return carry

    def back_rows(v, carry):
        high, low = split(back_y_here[pl.ds(v, 1), :] * all_z_here[:, : 2 * quarter])
        at = pl.ds(pl.multiple_of(v * grid_size, grid_size), grid_size)
        from_high[at, :] = high
        from_low[at, :] = low
        return carry

    lax.fori_loop(0, grid_size // 2, forward_rows, 0)
    lax.fori_loop(0, grid_size, back_rows, 0)
    for y in range(grid_size):
        pot_flat[:, y * grid_size:(y + 1) * grid_size] = pot_here[:, y, :]
    pot_flat[...] = shifted_potential(pot_flat[...], sites_here, grid_size) * (1.0 / (grid_size * cells))
    for place, v in enumerate(frequency_order(grid_size)):
        pot_order[:, place * grid_size:(place + 1) * grid_size] = pot_flat[:, int(v) * grid_size:(int(v) + 1) * grid_size]
    for x in range(grid_size):
        site_table[PART * x:PART * (x + 1), :] = jnp.broadcast_to(pot_order[x:x + 1, :], (PART, cells))

    pl.semaphore_wait(plane_sem, band_n - 1)

    quarters = [slice(i * quarter, (i + 1) * quarter) for i in range(4)]
    odd = slice(2 * quarter, 4 * quarter)
    lane = lax.broadcasted_iota(jnp.int32, (1, LANES), 1)
    tall = 2 * SUBLANES

    def lane_is(place):
        return lane == jnp.full((1, LANES), place, jnp.int32)

    def folded(product):
        return sum((product[i:i + SUBLANES] for i in range(SUBLANES, product.shape[0], SUBLANES)), product[:SUBLANES])

    def times_x(value):
        high, low = split(value)
        return jnp.dot(x_wide[...], jnp.concatenate([high, high, low], axis=0), preferred_element_type=jnp.float32)

    eighth = cells // 8
    early_columns = [pl.ds(sum(EARLY_EIGHTHS[:i]) * eighth, EARLY_EIGHTHS[i] * eighth) for i in range(len(EARLY_EIGHTHS))]
    early_stop = sum(EARLY_EIGHTHS) * eighth

    def early_copy(part, k):
        peer = (me + k) % n
        at = pl.ds(pl.multiple_of(peer * piece, SUBLANES), early)
        return pltpu.make_async_remote_copy(
            src_ref=basis.at[0, pl.ds(1, ITERS), at, early_columns[part]], dst_ref=early_land.at[me, :, :, early_columns[part]],
            send_sem=early_send.at[part, k], recv_sem=early_recv.at[part, k], device_id={"grid": peer}, device_id_type=MESH)

    def send_early(part):
        for k in range(1, n):
            early_copy(part, k).start()

    def message_copy(stage, k):
        return pltpu.make_async_remote_copy(
            src_ref=sums.at[stage, rank], dst_ref=sums.at[stage, rank], send_sem=sum_send.at[stage, k], recv_sem=sum_recv.at[stage, k],
            device_id={"grid": (me + k % n) % n, "band": (band + k // n) % band_n}, device_id_type=MESH)

    far_first = sorted(range(1, members), key=lambda k: -min(k // n, band_n - k // n))

    def send_message(stage, message):
        sums[stage, rank] = message
        for k in far_first:
            message_copy(stage, k).start()

    tiles = [slice(r, r + tall) for r in range(0, rows, tall)]

    def spread_quarters(at, q):
        even, other = q[0] + q[2], q[1] + q[3]
        for cols, value in zip(quarters, (even + other, even - other, q[0] - q[2], q[1] - q[3])):
            vec_high[at, cols], vec_low[at, cols] = split(value)

    def settle(t, results):
        alpha_part, square_part, norm, norm_before, message = results
        j = (t + ITERS - 1) % ITERS
        alpha = total_of([alpha_part]) * inverse_of(norm)
        gamma = jnp.where(jnp.full((1, 1), j, jnp.int32) == 0, 0.0, norm * inverse_of(norm_before))
        norm_after = jnp.maximum(total_of([square_part]) - alpha * alpha * norm - gamma * norm, 0.0)
        place = SUBLANES * ((t + ITERS - 1) // ITERS - 1) + j
        message = jnp.where(lane_is(place), norm, message)
        message = jnp.where(lane_is(place + 1), norm_after, message)
        message = jnp.where(lane_is(place + LANES // 2), alpha, message)
        return alpha, gamma, message

    def step(t, results, first=False, final=False):
        alpha, gamma, message = settle(t, results)
        group, j = t // ITERS, t % ITERS
        if first:
            for k in range(1, n):
                piece_copy(0, group, k).wait_recv()
            for at in tiles:
                spread_quarters(at, [basis[group, 0, at, cols] for cols in quarters])
        else:
            before, earlier, now = j - 1, jnp.maximum(j - 2, 0), j % 2

        def forward(i):
            cols = quarters[i]
            source, depth = (cols, quarter) if i < 2 else (odd, 2 * quarter)
            spectrum = dot3((vec_high[:, source], vec_low[:, source]), (to_high[:depth, cols], to_low[:depth, cols]))
            if first:
                past[0, :, cols] = spectrum
                past[1, :, cols] = jnp.zeros_like(spectrum)
            else:
                spectrum = spectrum - alpha * past[1 - now, :, cols] - gamma * past[now, :, cols]
                past[now, :, cols] = spectrum
            return spectrum

        def weigh(i, spectrum):
            return times_x(past[0 if first else now, :, quarters[i]]) * site_table[:, quarters[i]]

        def finish(i, spectrum):
            mid_high[:, quarters[i]], mid_low[:, quarters[i]] = split(times_x(spectrum))

        work = [forward(i) for i in range(4)]
        if final:
            send_message(0, message)
        work = [weigh(i, work[i]) for i in range(4)]
        for i in range(4):
            finish(i, work[i])
        norm_part = jnp.zeros((SUBLANES, quarter), jnp.float32)
        for at in tiles:
            for cols in quarters:
                value = basis[group, j, at, cols]
                if not first:
                    value = value - alpha * basis[group, before, at, cols] - gamma * basis[group, earlier, at, cols]
                    basis[group, j, at, cols] = value
                norm_part = norm_part + folded(value * value)
        norm = total_of([norm_part])
        if first:
            for k in range(1, n):
                piece_copy(1, group, k).wait_recv()
            if group == 1:
                send_early(0)

        def back(at, cols):
            return dot3((mid_high[:, at], mid_low[:, at]), (from_high[at, cols], from_low[at, cols]))

        zero, two = back(quarters[0], slice(0, quarter)), back(quarters[1], slice(0, quarter))
        odds = back(odd, slice(0, 2 * quarter))
        alpha_part, square_part = jnp.zeros((SUBLANES, quarter), jnp.float32), jnp.zeros((SUBLANES, quarter), jnp.float32)
        for at in tiles:
            plus, minus, one, three = zero[at] + two[at], zero[at] - two[at], odds[at, :quarter], odds[at, quarter:]
            q = []
            for cols, value in zip(quarters, (plus + one, minus + three, plus - one, minus - three)):
                here = basis[group, j, at, cols]
                new = energy[group, at, cols] * here - value
                basis[group, j + 1, at, cols] = new
                alpha_part = alpha_part + folded(here * new)
                square_part = square_part + folded(new * new)
                q.append(new)
            if not final:
                spread_quarters(at, q)
        return alpha_part, square_part, norm, results[2], message

    nothing, no_part = jnp.zeros((1, 1), jnp.float32), jnp.zeros((SUBLANES, quarter), jnp.float32)
    results = (no_part, no_part, nothing, nothing, jnp.zeros((1, LANES), jnp.float32))
    steps = GROUPS * ITERS
    for group in range(GROUPS):
        results = step(group * ITERS, results, first=True)
        stop = (group + 1) * ITERS - (group == GROUPS - 1)
        results = lax.fori_loop(group * ITERS + 1, stop, step, results)
    results = step(steps - 1, results, final=True)
    send_message(1, settle(steps, results)[2])
    send_early(1)

    def tables_of(stage):
        for k in range(1, members):
            message_copy(stage, k).wait_recv()
        for r in range(members):
            gathered[stage, r:r + 1, :] = sums[stage, r]
        table = gathered[stage]
        norms = jnp.where(wide_lane < LANES // 2, table, 0.0)
        return norms, pltpu.roll(table, LANES // 2, 1), jnp.where(order > 0, norms * inverse_of(pltpu.roll(norms, 1, 1)), 0.0)

    wide_lane = lax.broadcasted_iota(jnp.int32, (members, LANES), 1)
    order = wide_lane % SUBLANES
    used = jnp.logical_and(order <= ITERS, wide_lane < SUBLANES * GROUPS)

    def image_of(tables, vector):
        diagonal, coupling = tables[1:]
        raised = jnp.where(order > 0, pltpu.roll(vector, 1, 1), 0.0)
        lowered = jnp.where(order < ITERS, pltpu.roll(coupling * vector, LANES - 1, 1), 0.0)
        return jnp.where(used, raised + jnp.where(order < ITERS, diagonal, 0.0) * vector + lowered, 0.0)

    alphas, betas = jnp.zeros((1, LANES), jnp.float32), jnp.zeros((1, LANES), jnp.float32)
    tables = tables_of(0)
    vector, previous = jnp.where(jnp.logical_and(used, order == 0), 1.0, 0.0), jnp.zeros((members, LANES), jnp.float32)
    size = nothing
    for j in range(ITERS):
        if j == ITERS - 1:
            tables = tables_of(1)
        image = image_of(tables, vector)
        size_before, size = size, total_of([tables[0] * vector * vector])
        alpha = total_of([tables[0] * vector * image]) / size
        rest = image - alpha * vector
        if j > 0:
            ratio = size / size_before
            betas = jnp.where(lane == j - 1, jnp.sqrt(ratio), betas)
            rest = rest - ratio * previous
        alphas = jnp.where(lane == j, alpha, alphas)
        vector, previous = rest, vector
    norms, diagonal, coupling = tables
    top = ITERS - 1
    weights = vector - jnp.where(order == top, diagonal * pltpu.roll(vector, LANES - 1, 1), 0.0)
    weights = weights - jnp.where(order == top - 1, pltpu.roll(coupling, LANES - 1, 1) * pltpu.roll(vector, LANES - 2, 1), 0.0)
    size_before, size = size, total_of([norms * vector * vector])
    unit = 1.0 / jnp.sqrt(size / total_count)
    coef[0:1, :] = alphas
    coef[1:2, :] = jnp.where(lane == ITERS - 1, jnp.sqrt(size / size_before), betas)
    gathered[2] = weights

    def scales_of(owner):
        row = gathered[2, pl.ds(owner, 1), :]
        return [
            [jnp.sum(jnp.where(lane == SUBLANES * group + i, row, 0.0), axis=1, keepdims=True) * unit for i in range(ITERS + 1)]
            for group in range(GROUPS)
        ]

    scales = scales_of(rank)

    def own_value(group, at, cols):
        return sum((scales[group][i] * basis[group, i, at, cols] for i in range(1, ITERS + 1)), scales[group][0] * basis[group, 0, at, cols])

    every, late = slice(0, cells), slice(early_stop, cells)
    out_copies = []
    for k in [*range(n // 2 - 1, 0, -1), *range(n // 2, n + 1)]:
        peer = (me + k) % n
        here = pl.multiple_of(peer * piece, piece)
        target, place = (outgoing, peer) if k < n else (land, me)
        target[place, early:piece, :] = own_value(0, pl.ds(here + early, piece - early), every)
        target[place, piece:, :] = own_value(1, pl.ds(here, piece), every)
        if k == n:
            target[place, :early, :] = own_value(0, pl.ds(here, early), every)
            continue
        areas = [(pl.ds(early, GROUPS * piece - early), pl.ds(0, cells))]
        if early_stop < cells:
            target[place, :early, late] = own_value(0, pl.ds(here, early), late)
            areas.append((pl.ds(0, early), pl.ds(early_stop, cells - early_stop)))
        for i, (at, cols) in enumerate(areas):
            copy = pltpu.make_async_remote_copy(
                src_ref=outgoing.at[peer, at, cols], dst_ref=land.at[me, at, cols], send_sem=out_send.at[i, k], recv_sem=out_recv.at[i, k],
                device_id={"grid": peer}, device_id_type=MESH)
            copy.start()
            out_copies.append(copy)
    for k in range(1, n):
        for part in range(len(EARLY_EIGHTHS)):
            early_copy(part, k).wait()
        peer = (me + n - k) % n
        scale = scales_of(band * n + peer)[0]
        value = scale[0] * packed[0, 0, peer, :early, :early_stop]
        for i in range(1, ITERS + 1):
            value = value + scale[i] * early_land[peer, i - 1, :, :early_stop]
        land[peer, :early, :early_stop] = value
    for group in range(GROUPS):
        for kind in range(2):
            for k in range(1, n):
                piece_copy(kind, group, k).wait_send()
    for stage in range(2):
        for k in range(1, members):
            message_copy(stage, k).wait_send()
    for copy in out_copies:
        copy.wait()


def unpack_kernel(halves, planes, land, coef, out, alphas, betas):
    owners, cells = land.shape[0], land.shape[2]
    upper = lax.broadcasted_iota(jnp.int32, (SUBLANES, cells), 0) < PART
    for owner in range(owners):
        at = slice(owner % halves * SUBLANES, (owner % halves + 1) * SUBLANES)
        for pair in range(planes // 2):
            here = slice(pair * SUBLANES, (pair + 1) * SUBLANES)
            one, two = land[owner, here, :], land[owner, slice(here.start + planes * PART, here.stop + planes * PART), :]
            out[0, owner // halves, 0, at, 2 * pair * cells:(2 * pair + 1) * cells] = jnp.where(upper, one, pltpu.roll(two, PART, 0))
            out[0, owner // halves, 0, at, (2 * pair + 1) * cells:(2 * pair + 2) * cells] = jnp.where(upper, pltpu.roll(one, PART, 0), two)
    alphas[0] = coef[0:1, :ITERS]
    betas[0] = coef[1:2, :ITERS]


def field_body(start, energies, sites, potential):
    grid_size = potential.shape[0]
    cells = grid_size * grid_size
    n, band_n = lax.axis_size("grid"), lax.axis_size("band")
    halves = start.shape[3] // SUBLANES
    planes = grid_size // n
    rows, piece, half_cells = grid_size * PART, planes * PART, cells // 2
    index = np.arange(grid_size)
    angle = (index[:, None] * index[None, :] % grid_size) * (2.0 * math.pi / grid_size)
    cas = np.cos(angle) + np.sin(angle)
    ordered = cas[frequency_order(grid_size)]
    half_grid = grid_size // 2
    forward_y = jnp.asarray(np.repeat(ordered.T[:half_grid], grid_size, axis=1), jnp.float32)
    back_y = jnp.asarray(np.repeat(ordered[:, :half_grid], grid_size, axis=1), jnp.float32)
    all_z = jnp.asarray(np.tile(cas, (1, grid_size)), jnp.float32)
    x_wide = np.kron(cas, np.eye(PART)).astype(np.float32)
    x_high = x_wide.astype(jnp.bfloat16)
    x_low = (x_wide - x_high.astype(np.float32)).astype(jnp.bfloat16)
    x_wide = jnp.asarray(np.concatenate([x_high, x_low, x_high], axis=1))
    vmem = pl.BlockSpec(memory_space=pltpu.VMEM)
    hbm = pl.BlockSpec(memory_space=pltpu.MemorySpace.HBM)
    f32, bf16 = jnp.float32, jnp.bfloat16
    dma = pltpu.SemaphoreType.DMA
    members = n * band_n
    land_shape = (n, GROUPS * piece, cells)
    operands = (start, energies, sites[:, 0], potential, forward_y, back_y, all_z, x_wide)
    operands = (pltpu.with_memory_space_constraint(value, pltpu.MemorySpace.HBM) for value in operands)
    land, coef = pl.pallas_call(
        functools.partial(recursion_kernel, (n, band_n, grid_size, halves)),
        out_shape=(jax.ShapeDtypeStruct(land_shape, f32), jax.ShapeDtypeStruct((2, LANES), f32)),
        in_specs=[hbm] * 8,
        out_specs=(vmem, vmem),
        scratch_shapes=[
            pltpu.SMEM((3,), jnp.int32),
            pltpu.VMEM((half_grid, cells), f32), pltpu.VMEM((grid_size, half_cells), f32), pltpu.VMEM((grid_size, cells), f32),
            pltpu.VMEM((rows, 3 * rows), bf16), pltpu.VMEM(potential.shape, f32),
            pltpu.VMEM((grid_size, cells), f32), pltpu.VMEM((grid_size, cells), f32),
            pltpu.VMEM(start.shape, f32), pltpu.VMEM(energies.shape, f32),
            pltpu.VMEM((2, GROUPS, n, piece, cells), f32),
            pltpu.VMEM((GROUPS, ITERS + 1, rows, cells), f32), pltpu.VMEM((GROUPS, rows, cells), f32),
            pltpu.VMEM((rows, cells), f32),
            pltpu.VMEM((half_cells, cells), bf16), pltpu.VMEM((half_cells, cells), bf16),
            pltpu.VMEM((cells, half_cells), bf16), pltpu.VMEM((cells, half_cells), bf16),
            pltpu.VMEM((rows, cells), bf16), pltpu.VMEM((rows, cells), bf16),
            pltpu.VMEM((rows, cells), bf16), pltpu.VMEM((rows, cells), bf16),
            pltpu.VMEM((2, rows, cells), f32), pltpu.VMEM(land_shape, f32),
            pltpu.VMEM((n, ITERS, piece // 2, cells), f32),
            pltpu.VMEM((2, members, 1, LANES), f32), pltpu.VMEM((3, members, LANES), f32),
            dma((6,)), dma((2,)), dma((2, GROUPS, n)), dma((2, GROUPS, n)), dma((2, n)), dma((2, n)),
            dma((2, members)), dma((2, members)), pltpu.SemaphoreType.REGULAR, dma((len(EARLY_EIGHTHS), n)), dma((len(EARLY_EIGHTHS), n)),
        ],
        compiler_params=pltpu.CompilerParams(collective_id=0, has_side_effects=True, vmem_limit_bytes=36 * 1024 * 1024),
    )(*operands)
    scalar = jax.ShapeDtypeStruct((1, 1, ITERS), f32)
    out, alphas, betas = pl.pallas_call(
        functools.partial(unpack_kernel, halves, planes),
        out_shape=(jax.ShapeDtypeStruct(start.shape, f32), scalar, scalar),
        in_specs=[vmem, vmem],
        out_specs=(vmem, vmem, vmem),
        compiler_params=pltpu.CompilerParams(vmem_limit_bytes=8 * 1024 * 1024),
    )(land, coef)
    return alphas, betas, out


def body(start, energies, sites, potential):
    atoms, cores, pols, bands, _ = start.shape
    grid_size = potential.shape[0]
    n = lax.axis_size("grid")
    whole_fields = (
        atoms == 1 and pols == 1 and bands % SUBLANES == 0 and cores * bands == SUBLANES * n
        and grid_size % (2 * SUBLANES) == 0 and grid_size % (2 * n) == 0
        and grid_size * grid_size % (4 * LANES) == 0 and n * lax.axis_size("band") % SUBLANES == 0
    )
    return (field_body if whole_fields else plane_body)(start, energies, sites, potential)


def solution(mesh):
    in_specs = (P(None, None, None, "band", "grid"), P(None, "band", "grid"), P(), P())
    out_specs = (P(), P(), P(None, None, None, "band", "grid"))
    return jax.shard_map(body, mesh=mesh, in_specs=in_specs, out_specs=out_specs, check_vma=False)
```
